32 devices in a mesh: dp: 8 (over z, y), seq: 4 (over x, core).
Axes of the slice: x: 2, y: 2, z: 4, core: 2. Of those that a mesh axis runs over, the one named last changes fastest.
Arguments:
- decoder_in: bfloat16 [8, 512, 1024], P('dp', 'seq'), may hold values from -6 to 6
- encoder_states: bfloat16 [8, 1024, 1024], P('dp', 'seq'), may hold values from -6 to 6
- out_grad: bfloat16 [8, 512, 1024], P('dp', 'seq'), may hold values from -6 to 6
- seq_lengths: int32 [8], P('dp'), may hold values from 128 to 512, as said below
- enc_lengths: int32 [8], P('dp'), may hold values from 256 to 1024, as said below
- self_qkv: bfloat16 [3, 1024, 1024], P(None, 'dp'), may hold values from -0.1875 to 0.1875
- self_out: bfloat16 [1024, 1024], P('dp'), may hold values from -1.5 to 1.5
- cross_qkv: bfloat16 [3, 1024, 1024], P(None, 'dp'), may hold values from -0.1875 to 0.1875
- cross_out: bfloat16 [1024, 1024], P('dp'), may hold values from -1.5 to 1.5
- attn_bias: bfloat16 [6, 1024], P(None, 'dp'), may hold values from -3 to 3
- ffn_in: bfloat16 [1024, 4096], P('dp'), may hold values from -0.1875 to 0.1875
- ffn_in_bias: bfloat16 [4096], P('dp'), may hold values from -3 to 3
- ffn_out: bfloat16 [4096, 1024], P('dp'), may hold values from -0.09375 to 0.09375
- ffn_out_bias: bfloat16 [1024], P('dp'), may hold values from -3 to 3
- norm_gain: bfloat16 [3, 1024], P(None, 'dp'), may hold values from 0.5 to 1.5
- norm_bias: bfloat16 [3, 1024], P(None, 'dp'), may hold values from -2 to 2
Outputs:
- layer_out: bfloat16 [8, 512, 1024], P('dp', 'seq')
- grad_input: bfloat16 [8, 512, 1024], P('dp', 'seq')
- grad_encoder: bfloat16 [8, 1024, 1024], P('dp', 'seq')
- grad_self_qkv: float32 [3, 1024, 1024], P(None, 'dp')
- grad_self_out: float32 [1024, 1024], P('dp')
- grad_cross_qkv: float32 [3, 1024, 1024], P(None, 'dp')
- grad_cross_out: float32 [1024, 1024], P('dp')
- grad_attn_bias: float32 [6, 1024], P(None, 'dp')
- grad_ffn_in: float32 [1024, 4096], P('dp')
- grad_ffn_in_bias: float32 [4096], P('dp')
- grad_ffn_out: float32 [4096, 1024], P('dp')
- grad_ffn_out_bias: float32 [1024], P('dp')
- grad_norm_gain: float32 [3, 1024], P(None, 'dp')
- grad_norm_bias: float32 [3, 1024], P(None, 'dp')
The draws below stay inside these ranges and needn't reach their ends.
Inputs may be any that keep to these rules, and one draw needn't show every extreme that they name: Sequence s has seq_lengths[s] real positions at its start, the rest is padding; some sequence is full. Sequence s has enc_lengths[s] real encoder positions at its start; some sequence's encoder states are full.
All inputs are finite; a program needn't handle non-finite values.
Results may differ from the reference program's by a relative error of at most 0.033.
Values may be sent and summed in bfloat16 or wider, within the bound.
A program may use at most 320 MiB of HBM per device.

```python
import jax
import jax.numpy as jnp
from jax import lax

H = 16
HD = 64
D = 1024
FF = 4096
L = 512
E = 1024
SEQS = 8


def draw_seq_lengths(key, part):
    drawn_lengths = jax.random.randint(key, (SEQS,), L // 4, L + 1)
    longest = jax.random.randint(jax.random.fold_in(key, 7), (), 0, SEQS)
    return jnp.where(jnp.arange(SEQS) == longest, L, drawn_lengths).astype(jnp.int32)


def draw_enc_lengths(key, part):
    drawn_lengths = jax.random.randint(key, (SEQS,), E // 4, E + 1)
    longest = jax.random.randint(jax.random.fold_in(key, 11), (), 0, SEQS)
    return jnp.where(jnp.arange(SEQS) == longest, E, drawn_lengths).astype(jnp.int32)


def with_spikes(entries, rng, source, target, shards_of, factor):
    def block_of(position):
        return (jnp.arange(entries.shape[position]) // (entries.shape[position] // shards_of)).reshape((-1,) + (1,) * (entries.ndim - 1 - position))

    first = jax.random.permutation(rng, shards_of)[block_of(target)]
    other_side = (block_of(target) + shards_of // 2) % shards_of
    return jnp.where((block_of(source) == first) | (block_of(source) == other_side), factor * entries, entries)


def shard_levels(own_key, extent, pieces, low, high):
    def one(axis_at, blocks):
        heights = jax.random.uniform(jax.random.fold_in(jax.random.fold_in(own_key, 6), axis_at), (blocks,), jnp.float32, low / len(pieces), high / len(pieces))
        return jnp.repeat(jnp.exp(heights), extent[axis_at] // blocks).reshape((-1,) + (1,) * (len(extent) - axis_at - 1))

    loudness = one(*pieces[0])
    for cut in pieces[1:]:
        loudness = loudness * one(*cut)
    return loudness


def noise(stream_key, shape, width, reach, split=(), kind=jnp.bfloat16):
    loudness = shard_levels(stream_key, shape, split, -0.22, 0.18) if split else 1.0
    drawn = jax.random.normal(stream_key, shape, jnp.float32) * width * loudness
    return jnp.minimum(jnp.maximum(drawn, -reach), reach).astype(kind)


def noise_with(stream_key, extent, deviation, most, cuts, heavy, held_as=jnp.bfloat16):
    values = deviation * jax.random.normal(stream_key, extent, jnp.float32)
    if cuts:
        values = values * shard_levels(stream_key, extent, cuts, -0.22, 0.18)
    return jnp.clip(with_spikes(values, jax.random.fold_in(stream_key, 3), *heavy), -most, most).astype(held_as)


def setup_inputs(seed: int = 0) -> dict:
    seeds = jax.random.split(jax.random.key(seed), 17)
    decoder_in = noise_with(seeds[0], (SEQS, L, D), 1.0, 6.0, ((0, 8), (1, 4)), (0, 2, 8, 2.0))
    encoder_states = noise(seeds[1], (SEQS, E, D), 1.0, 6.0, ((0, 8), (1, 4)))
    out_grad = noise(seeds[2], (SEQS, L, D), 1.0, 6.0, ((0, 8), (1, 4)))
    seq_lengths = draw_seq_lengths(jax.random.fold_in(seeds[16], 71), 0)
    enc_lengths = draw_enc_lengths(jax.random.fold_in(seeds[16], 71), 0)
    self_qkv = noise(seeds[5], (3, D, D), D ** -0.5, 0.1875, ((1, 8),))
    self_out = noise(seeds[6], (D, D), (D // 64) ** -0.5, 1.5, ((0, 8),))
    cross_qkv = noise(seeds[7], (3, D, D), D ** -0.5, 0.1875, ((1, 8),))
    cross_out = noise(seeds[8], (D, D), (D // 64) ** -0.5, 1.5, ((0, 8),))
    attn_bias = noise(seeds[9], (6, D), 0.5, 3.0, ((1, 8),))
    ffn_in = noise(seeds[10], (D, FF), D ** -0.5, 0.1875, ((0, 8),))
    ffn_in_bias = noise(seeds[11], (FF,), 0.5, 3.0, ((0, 8),))
    ffn_out = noise(seeds[12], (FF, D), FF ** -0.5, 0.09375, ((0, 8),))
    ffn_out_bias = noise(seeds[13], (D,), 0.5, 3.0, ((0, 8),))
    norm_gain = jnp.clip(1.0 + 0.1 * jax.random.normal(seeds[14], (3, D), jnp.float32), 0.5, 1.5).astype(jnp.bfloat16)
    norm_bias = noise(seeds[15], (3, D), 0.3, 2.0, ((1, 8),))
    return {"decoder_in": decoder_in, "encoder_states": encoder_states, "out_grad": out_grad, "seq_lengths": seq_lengths, "enc_lengths": enc_lengths, "self_qkv": self_qkv, "self_out": self_out, "cross_qkv": cross_qkv, "cross_out": cross_out, "attn_bias": attn_bias, "ffn_in": ffn_in, "ffn_in_bias": ffn_in_bias, "ffn_out": ffn_out, "ffn_out_bias": ffn_out_bias, "norm_gain": norm_gain, "norm_bias": norm_bias}


@jax.custom_vjp
def low(v):
    return lax.optimization_barrier(v.astype(jnp.bfloat16)).astype(jnp.float32)

@jax.custom_vjp
def low_back(v):
    return v

def low_keep(v):
    return (low(v), None)

def low_pass(kept, grad):
    return (grad,)

def back_keep(v):
    return (v, None)

def back_low(kept, grad):
    return (low(grad),)
low.defvjp(low_keep, low_pass)
low_back.defvjp(back_keep, back_low)
norm_eps = 1e-05

def matmul(left, right):
    return jnp.dot(left, right, precision=lax.Precision.HIGHEST)

def layer_norm(inputs, gain_row, shift_row):
    row_mean = lax.optimization_barrier(jnp.mean(inputs, axis=-1, keepdims=True))
    centred = inputs - row_mean
    variance = lax.optimization_barrier(jnp.mean(centred * centred, axis=-1, keepdims=True))
    return centred * lax.rsqrt(variance + norm_eps) * gain_row + shift_row

def gelu_exact(pre_values):
    return 0.5 * pre_values * (1.0 + lax.erf(pre_values * 0.7071067811865476))

def attention(queries, keys_in, values_in, causal, key_limit):
    block_rows = min(512, L)
    block_count = L // block_rows
    score_scale = HD ** (-0.5)
    keys3 = keys_in.reshape(keys_in.shape[0], H, HD)
    values3 = values_in.reshape(values_in.shape[0], H, HD)
    col_ids = jnp.arange(keys_in.shape[0], dtype=jnp.int32)
    q_blocks = queries.reshape(block_count, block_rows, H, HD)
    starts = jnp.arange(block_count, dtype=jnp.int32) * block_rows

    def block_fn(block_item):
        start_row, q_block = block_item
        row_ids = start_row + jnp.arange(block_rows, dtype=jnp.int32)
        if causal:
            allowed = col_ids[None, :] <= row_ids[:, None]
        else:
            allowed = jnp.broadcast_to(col_ids[None, :] < key_limit, (block_rows, col_ids.shape[0]))
        scores = jnp.einsum('qhd,khd->hqk', q_block, keys3, precision=lax.Precision.HIGHEST) * score_scale
        scores = low_back(scores)
        scores = jnp.where(allowed[None], scores, -1e+30)
        row_top = lax.optimization_barrier(jnp.max(scores, axis=-1, keepdims=True))
        expo_terms = jnp.exp(scores - row_top)
        probabilities = expo_terms / lax.optimization_barrier(jnp.sum(expo_terms, axis=-1, keepdims=True))
        probabilities = low(probabilities)
        block_out = jnp.einsum('hqk,khd->qhd', probabilities, values3, precision=lax.Precision.HIGHEST)
        return block_out.reshape(block_rows, H * HD)
    outputs = lax.map(jax.checkpoint(block_fn), (starts, q_blocks))
    return outputs.reshape(L, H * HD)

def forward(params, x_seq, enc_seq, seq_len, enc_len):
    self_qkv, self_out, cross_qkv, cross_out, attn_bias, ffn_in, ffn_in_bias, ffn_out, ffn_out_bias, norm_gain, norm_bias = params
    row_ids = jnp.arange(L, dtype=jnp.int32)
    self_q = low_back(low(matmul(x_seq, self_qkv[0]) + attn_bias[0]))
    self_k = low_back(low(matmul(x_seq, self_qkv[1])))
    self_v = low_back(low(matmul(x_seq, self_qkv[2]) + attn_bias[1]))
    self_o = low_back(low(attention(self_q, self_k, self_v, True, seq_len)))
    branch = low_back(matmul(self_o, self_out) + attn_bias[2])
    first_out = layer_norm(x_seq + branch, norm_gain[0], norm_bias[0])
    first_low = low(first_out)
    cross_q = low_back(low(matmul(first_low, cross_qkv[0]) + attn_bias[3]))
    cross_k = low_back(low(matmul(enc_seq, cross_qkv[1])))
    cross_v = low_back(low(matmul(enc_seq, cross_qkv[2]) + attn_bias[4]))
    cross_o = low_back(low(attention(cross_q, cross_k, cross_v, False, enc_len)))
    branch_two = low_back(matmul(cross_o, cross_out) + attn_bias[5])
    second = layer_norm(first_out + branch_two, norm_gain[1], norm_bias[1])
    pre_act = low_back(matmul(low(second), ffn_in) + ffn_in_bias)
    hidden = low(gelu_exact(pre_act))
    branch_three = low_back(matmul(hidden, ffn_out) + ffn_out_bias)
    third_out = layer_norm(second + branch_three, norm_gain[2], norm_bias[2])
    return third_out * (row_ids < seq_len).astype(jnp.float32)[:, None]

def reference(decoder_in, encoder_states, out_grad, seq_lengths, enc_lengths, self_qkv, self_out, cross_qkv, cross_out, attn_bias, ffn_in, ffn_in_bias, ffn_out, ffn_out_bias, norm_gain, norm_bias):
    params = tuple((weight_arr.astype(jnp.float32) for weight_arr in (self_qkv, self_out, cross_qkv, cross_out, attn_bias, ffn_in, ffn_in_bias, ffn_out, ffn_out_bias, norm_gain, norm_bias)))
    totals = tuple((jnp.zeros(weight_arr.shape, jnp.float32) for weight_arr in params))

    def per_sequence(carry_in, seq_items):
        x_seq, enc_seq, cot_seq, seq_len, enc_len = seq_items

        def local_forward(weight_set, x_value, enc_value):
            return forward(weight_set, x_value, enc_value, seq_len, enc_len)
        seq_out, pullback = jax.vjp(local_forward, params, x_seq.astype(jnp.float32), enc_seq.astype(jnp.float32))
        grad_params, grad_x, grad_enc = pullback(cot_seq.astype(jnp.float32))
        summed = tuple((total_a + grad_b for total_a, grad_b in zip(carry_in, grad_params)))
        return (summed, (seq_out.astype(jnp.bfloat16), grad_x.astype(jnp.bfloat16), grad_enc.astype(jnp.bfloat16)))
    totals, stacked = lax.scan(per_sequence, totals, (decoder_in, encoder_states, out_grad, seq_lengths, enc_lengths))
    layer_out, grad_input, grad_encoder = stacked
    return (layer_out, grad_input, grad_encoder, totals[0], totals[1], totals[2], totals[3], totals[4], totals[5], totals[6], totals[7], totals[8], totals[9], totals[10])
```

```python
import functools
import types

import jax
import jax.numpy as jnp
from jax import lax
from jax.experimental import pallas as pl
from jax.experimental.pallas import tpu as pltpu
from jax.sharding import PartitionSpec as P

HD = 64
EPS = 1e-05
F32 = jnp.float32
BF = jnp.bfloat16
MESH = pl.DeviceIdType.MESH
ANY = pl.BlockSpec(memory_space=pl.ANY)
CH = 256
NS = 32
DP = "dp"
SEQ = "seq"
LO = "lo"
SMALL = "small"
LENS = "lens"
FIRST = "x"
FJ_MAX = 4096
AHEAD = 2
AHEAD_Y = 2
PLAN = (1, 1, 1, 1, 2, 1, 1, 1, 1, 1, 1, 0)
BPLAN = (0, 1, 1, 1, 0, 1, 2, 1, 1, 0, 1, 0, 1, 0, 1, 1, 1, 0, 1, 1)
PROBS = ("pbs", "pbc")


def configure(R, S, Tl, El, D, FF):
    g = types.SimpleNamespace(R=R, S=S, Tl=Tl, El=El, D=D, FF=FF)
    g.Y = 1
    while 8 * g.Y * g.Y <= R:
        g.Y *= 2
    g.Z = R // g.Y
    g.X = S // 2
    g.Dl = D // R
    g.FR = FF // R
    g.FB = g.FR // S
    g.DH = D // S
    g.FJ = FF // S
    g.NB = g.DH // 128
    g.H = g.DH // HD
    g.L = Tl * S
    g.E = El * S
    g.wide = g.Dl == 128 and g.FB == 128
    return g


def dot(a, b):
    return jnp.dot(a, b, preferred_element_type=F32)


def dot_nt(a, b):
    return lax.dot_general(a, b, (((1,), (1,)), ((), ())), preferred_element_type=F32)


def dot_tn(a, b):
    return lax.dot_general(a, b, (((0,), (0,)), ((), ())), preferred_element_type=F32)


def rem(a, b):
    return lax.rem(a, jnp.int32(b))


def at(start, size):
    if isinstance(start, int):
        return pl.ds(start, size)
    return pl.ds(pl.multiple_of(start, size), size)


def loop(count, body):
    if count == 1:
        body(0)
    else:
        lax.fori_loop(0, count, lambda n, z: (body(n), z)[1], 0)


def project(dst, a, w, transposed=False):
    def body(n):
        cols = at(n * 256, 256)
        dst[:, cols] = dot_nt(a, w[cols, :]) if transposed else dot(a, w[:, cols])

    loop(dst.shape[1] // 256, body)


def normalise(v):
    c = v - jnp.mean(v, axis=-1, keepdims=True)
    rstd = lax.rsqrt(jnp.mean(c * c, axis=-1, keepdims=True) + EPS)
    return c * rstd, rstd


class Comm:
    def __init__(self, g, r):
        self.g, self.r = g, r
        self.i = lax.axis_index(DP)
        self.j = lax.axis_index(SEQ)
        self.z, self.y = self.i // g.Y, rem(self.i, g.Y)
        self.x, self.c = self.j // 2, rem(self.j, 2)
        self.pending = []

    def zpeer(self, d):
        return (rem(self.z + d, self.g.Z) * self.g.Y + self.y, self.j)

    def ypeer(self, d):
        return (self.z * self.g.Y + rem(self.y + d, self.g.Y), self.j)

    def xpeer(self, d):
        return (self.i, rem(self.x + d, self.g.X) * 2 + self.c)

    def partner(self):
        return (self.i, self.x * 2 + 1 - self.c)

    def barrier(self):
        g = self.g
        peers = [self.zpeer(d) for d in range(1, g.Z)]
        peers += [self.ypeer(d) for d in range(1, g.Y)]
        peers += [self.xpeer(d) for d in range(1, g.X)]
        peers.append(self.partner())
        sem = pltpu.get_barrier_semaphore()
        for p in peers:
            pl.semaphore_signal(sem, inc=1, device_id=p, device_id_type=MESH)
        pl.semaphore_wait(sem, len(peers))

    def copy(self, src, dst, ss, rs, dev):
        return pltpu.make_async_remote_copy(
            src_ref=src, dst_ref=dst, send_sem=ss, recv_sem=rs, device_id=dev, device_id_type=MESH
        )

    def local(self, src, dst, sem):
        d = pltpu.make_async_copy(src, dst, sem)
        d.start()
        return d

    def when(self, cond, fn):
        if cond is None:
            fn()
        else:
            pl.when(cond)(fn)

    def w_descs(self, p, view, dz):
        r, g = self.r, self.g
        i = rem(self.z - dz + g.Z, g.Z) * g.Y + self.y
        v = view(i)
        return i, [
            self.copy(v, v, r.wys.at[p, d - 1, dz], r.wyr.at[p, d - 1, dz], self.ypeer(d))
            for d in range(1, g.Y)
        ]

    def w_z(self, p, view, d):
        v = view(self.i)
        r = self.r
        return self.copy(v, v, r.wzs.at[p, d - 1], r.wzr.at[p, d - 1], self.zpeer(d))

    def w_start(self, p, view, own=lambda i: None):
        def go():
            for d in range(1, self.g.Z):
                self.w_z(p, view, d).start()

        self.when(own(self.i), go)

    def w_relay(self, p, view, own=lambda i: None):
        r, g = self.r, self.g
        for dz in range(g.Z):
            i, descs = self.w_descs(p, view, dz)

            def go(i=i, descs=descs, dz=dz):
                v = view(i)
                if dz:
                    self.copy(
                        v, v, r.wzs.at[p, dz - 1], r.wzr.at[p, dz - 1], self.zpeer(dz)
                    ).wait_recv()
                for d in descs:
                    d.start()

            self.when(own(i), go)

    def w_finish(self, p, view, own=lambda i: None):
        r, g = self.r, self.g
        for dz in range(g.Z):
            for d in range(1, g.Y):
                i = rem(self.z - dz + g.Z, g.Z) * g.Y + rem(self.y - d + g.Y, g.Y)

                def go(i=i, d=d, dz=dz):
                    v = view(i)
                    self.copy(
                        v, v, r.wys.at[p, d - 1, dz], r.wyr.at[p, d - 1, dz], self.ypeer(d)
                    ).wait_recv()

                self.when(own(i), go)

    def w_drain(self, p, view, own=lambda i: None):
        g = self.g

        def go():
            for d in range(1, g.Z):
                self.w_z(p, view, d).wait_send()

        self.when(own(self.i), go)
        for dz in range(g.Z):
            i, descs = self.w_descs(p, view, dz)

            def go2(descs=descs):
                for d in descs:
                    d.wait_send()

            self.when(own(i), go2)

    def ag_x(self, k, view, d):
        v, r = view(self.j), self.r
        return self.copy(v, v, r.axs.at[k, d - 1], r.axr.at[k, d - 1], self.xpeer(d))

    def ag_c(self, k, view, d):
        g, r = self.g, self.r
        v = view(rem(self.x - d + g.X, g.X) * 2 + self.c)
        return self.copy(v, v, r.acs.at[k, d], r.acr.at[k, d], self.partner())

    def ag_start(self, k, view):
        for d in range(1, self.g.X):
            self.ag_x(k, view, d).start()
        self.ag_c(k, view, 0).start()

    def ag_relay(self, k, view):
        g, r = self.g, self.r
        for d in range(1, g.X):
            v = view(rem(self.x - d + g.X, g.X) * 2 + self.c)
            self.copy(
                v, v, r.axs.at[k, d - 1], r.axr.at[k, d - 1], self.xpeer(d)
            ).wait_recv()
            self.ag_c(k, view, d).start()

    def ag_finish(self, k, view):
        g, r = self.g, self.r
        for d in range(g.X):
            v = view(rem(self.x - d + g.X, g.X) * 2 + 1 - self.c)
            self.copy(v, v, r.acs.at[k, d], r.acr.at[k, d], self.partner()).wait_recv()

    def ag_drain(self, k, view):
        for d in range(1, self.g.X):
            self.ag_x(k, view, d).wait_send()
        for d in range(self.g.X):
            self.ag_c(k, view, d).wait_send()

    def rs_c(self, k, b, d):
        r = self.r
        return self.copy(
            b.ps.at[d], b.pr.at[d], r.rcs.at[k, d], r.rcr.at[k, d], self.partner()
        )

    def rs_x(self, k, b, d):
        r = self.r
        return self.copy(
            b.xs.at[d - 1],
            b.xr.at[d - 1],
            r.rxs.at[k, d - 1],
            r.rxr.at[k, d - 1],
            self.xpeer(d),
        )

    def rs_start(self, k, b, n, part):
        g = self.g
        for d in list(range(1, g.X)) + [0]:
            part(rem(self.x + d, g.X), b.part)
            b.acc[d] = b.part[at(self.c * n, n), :]
            b.ps[d] = b.part[at((1 - self.c) * n, n), :].astype(BF)
            self.rs_c(k, b, d).start()
        self.rs_turn(k, b)

    def rs_start_halves(self, k, b, n, part):
        g = self.g
        for d in list(range(1, g.X)) + [0]:
            first = rem(self.x + d, g.X) * 2 * n
            b.ps[d] = part(at(first + (1 - self.c) * n, n)).astype(BF)
            self.rs_c(k, b, d).start()
            b.acc[d] = part(at(first + self.c * n, n)).astype(b.acc.dtype)

    def rs_turn(self, k, b):
        for d in range(1, self.g.X):
            self.rs_c(k, b, d).wait_recv()
            b.xs[d - 1] = (b.acc[d][...].astype(F32) + b.pr[d].astype(F32)).astype(BF)
            self.rs_x(k, b, d).start()

    def rs_finish(self, k, b):
        g = self.g
        self.rs_c(k, b, 0).wait_recv()
        total = b.acc[0][...].astype(F32) + b.pr[0].astype(F32)
        for d in range(1, g.X):
            self.rs_x(k, b, d).wait_recv()
            total = total + b.xr[d - 1].astype(F32)
        for d in range(g.X):
            self.rs_c(k, b, d).wait_send()
        for d in range(1, g.X):
            self.rs_x(k, b, d).wait_send()
        return total

    def g_y(self, t, d, dz):
        g, r = self.g, self.r
        p, view, yr, zr, out = t
        i = rem(self.z + dz, g.Z) * g.Y + rem(self.y + d, g.Y)
        return self.copy(
            view(i),
            yr.at[d - 1, dz],
            r.gys.at[p, d - 1, dz],
            r.gyr.at[p, d - 1, dz],
            self.ypeer(d),
        )

    def g_z(self, t, dz):
        g, r = self.g, self.r
        p, view, yr, zr, out = t
        i = rem(self.z + dz, g.Z) * g.Y + self.y
        return self.copy(
            view(i), zr.at[dz - 1], r.gzs.at[p, dz - 1], r.gzr.at[p, dz - 1], self.zpeer(dz)
        )

    def g_start(self, t):
        for dz in list(range(1, self.g.Z)) + [0]:
            for d in range(1, self.g.Y):
                self.g_y(t, d, dz).start()

    def g_sum(self, t, dz):
        g = self.g
        p, view, yr, zr, out = t
        v = view(rem(self.z + dz, g.Z) * g.Y + self.y)
        total = v[...].astype(F32)
        for d in range(1, g.Y):
            self.g_y(t, d, dz).wait_recv()
            total = total + yr[d - 1, dz].astype(F32)
        return v, total

    def g_turn(self, t):
        for dz in range(1, self.g.Z):
            v, total = self.g_sum(t, dz)
            v[...] = total.astype(v.dtype)
            self.g_z(t, dz).start()

    def g_finish(self, t):
        p, view, yr, zr, out = t
        v, total = self.g_sum(t, 0)
        for dz in range(1, self.g.Z):
            self.g_z(t, dz).wait_recv()
            total = total + zr[dz - 1].astype(F32)
        out[...] = total.astype(out.dtype)

    def g_drain(self, t):
        for dz in range(self.g.Z):
            for d in range(1, self.g.Y):
                self.g_y(t, d, dz).wait_send()
        for dz in range(1, self.g.Z):
            self.g_z(t, dz).wait_send()


def attend_forward(g, q_ref, k_ref, v_ref, o_ref, p_ref, Lk, causal, limit, between):
    lane = lax.broadcasted_iota(jnp.int32, (1, 128), 1)
    low = lane < HD
    scale = HD ** -0.5
    for a in range(g.L // CH):
        rows = pl.ds(a * CH, CH)
        kk = (a + 1) * CH if causal else Lk
        keys = pl.ds(0, kk)
        col = lax.broadcasted_iota(jnp.int32, (CH, kk), 1)
        if causal:
            ok = col <= lax.broadcasted_iota(jnp.int32, (CH, kk), 0) + a * CH
        else:
            ok = col < limit

        def body(t):
            cols = at(t * 128, 128)
            q = q_ref[rows, cols]
            k = k_ref[keys, cols]
            v = v_ref[keys, cols]
            outs = []
            for e in range(2):
                qe = jnp.where(low if e == 0 else ~low, q, jnp.zeros_like(q))
                s = jnp.where(ok, dot_nt(qe, k) * scale, -1e30)
                ex = jnp.exp(s - jnp.max(s, axis=-1, keepdims=True))
                pb = (ex * (1.0 / jnp.sum(ex, axis=-1, keepdims=True))).astype(BF)
                p_ref[2 * t + e, rows, keys] = pb
                outs.append(dot(pb, v))
            o_ref[rows, cols] = jnp.where(low, outs[0], outs[1]).astype(BF)

        loop(g.NB, body)
        between(a)


def forward_kernel(g, names, *refs):
    r = types.SimpleNamespace(**dict(zip(names, refs)))
    cm = Comm(g, r)
    i, j, x, c = cm.i, cm.j, cm.x, cm.c
    Tl, El, D, Dl, DH, FB = g.Tl, g.El, g.D, g.Dl, g.DH, g.FB

    xv = lambda s: r.x.at[at(s * Tl, Tl), :]
    ev = lambda s: r.enc.at[at(s * El, El), :]
    lx = cm.local(r.tok, xv(j), r.ls.at[0])
    le = cm.local(r.states, ev(j), r.ls.at[1])

    own_rows = at(i * Dl, Dl)

    def col_block(t):
        return pl.ds(pl.multiple_of((t * g.S + j) * 128, 128), 128)

    def stage3(src, dst, sem):
        return [
            cm.local(
                src.at[:, :, col_block(t)], dst.at[:, own_rows, pl.ds(t * 128, 128)], sem.at[t]
            )
            for t in range(g.NB)
        ]

    def so_row(s):
        b = (s * Dl) // 128
        return (b // g.S) * 128 + rem(s * Dl, 128)

    def so_own(s):
        return rem((s * Dl) // 128, g.S) == j

    views = {}
    pieces = []

    def piece(view, own=lambda s: None):
        pieces.append((len(pieces), view, own))
        return pieces[-1]

    if g.wide:
        p_small = piece(lambda s: r.smalls.at[s])
    p_q = [piece(lambda s, n=n: r.wq.at[n, at(s * Dl, Dl), :]) for n in range(3)]
    p_so = piece(lambda s: r.wo.at[at(so_row(s), Dl), :], so_own)
    p_c = [piece(lambda s, n=n: r.wc.at[n, at(s * Dl, Dl), :]) for n in range(3)]
    p_co = piece(lambda s: r.wd.at[at(so_row(s), Dl), :], so_own)
    n1 = g.FJ // 256
    p_1 = [
        piece(lambda s, n=n: r.w1.at[at(s * Dl, Dl), pl.ds(n * 256, 256)]) for n in range(n1)
    ]
    n2 = D // 256
    p_2 = [
        piece(lambda s, n=n: r.w2.at[at(s * FB, FB), pl.ds(n * 256, 256)]) for n in range(n2)
    ]

    st_q = stage3(r.self_qkv, r.wq, r.lq)
    if g.wide:
        f = r.mine
        f[...] = jnp.zeros_like(f)
        nf = g.FF // D
        f[0:6, :] = r.attn_bias[...].astype(F32)
        f[6 : 6 + nf, :] = r.ffn_in_bias[...].astype(F32)
        f[6 + nf : 7 + nf, :] = r.ffn_out_bias[...].astype(F32)
        f[7 + nf : 10 + nf, :] = r.norm_gain[...].astype(F32)
        f[10 + nf : 13 + nf, :] = r.norm_bias[...].astype(F32)
        r.smalls[i] = f[...].astype(BF)

    def stage_row(src, dst, sem, wait):
        def go():
            d = pltpu.make_async_copy(src, dst.at[at(so_row(i), Dl), :], sem)
            if wait:
                d.wait()
            else:
                d.start()

        pl.when(so_own(i))(go)

    stage_row(r.self_out, r.wo, r.ls.at[3], False)
    st_c = stage3(r.cross_qkv, r.wc, r.lc)
    stage_row(r.cross_out, r.wd, r.ls.at[4], False)
    if g.wide:
        st_1 = [
            cm.local(
                r.ffn_in.at[:, pl.ds(pl.multiple_of((t * g.S + j) * 128, 128), 128)],
                r.w1.at[own_rows, pl.ds(t * 128, 128)],
                r.l1.at[t],
            )
            for t in range(g.R)
        ]
    else:
        st_1 = [cm.local(r.ffn_in, r.w1.at[own_rows, :], r.l1.at[0])]
    st_2 = [
        cm.local(r.ffn_out.at[at(j * FB, FB), :], r.w2.at[at(i * FB, FB), :], r.ls.at[5])
    ]

    cm.barrier()

    lx.wait()
    cm.ag_start(0, xv)
    staged = []
    for n in range(3):
        staged.append((p_q[n], st_q if n == 0 else [], None))
    staged.append((p_so, [], (r.self_out, r.wo, r.ls.at[3])))
    for n in range(3):
        staged.append((p_c[n], st_c if n == 0 else [], None))
    staged.append((p_co, [], (r.cross_out, r.wd, r.ls.at[4])))
    for n in range(n1):
        staged.append((p_1[n], st_1 if n == 0 else [], None))
    for n in range(n2):
        staged.append((p_2[n], st_2 if n == 0 else [], None))

    def start_next():
        if staged:
            p, descs, own_rows_copy = staged.pop(0)
            for d in descs:
                d.wait()
            if own_rows_copy:
                stage_row(*own_rows_copy, True)
            cm.w_start(*p)

    if g.wide:
        cm.w_start(*p_small)
    for _ in range(AHEAD):
        start_next()
    if g.wide:
        cm.w_relay(*p_small)
    cm.ag_relay(0, xv)
    le.wait()
    cm.ag_start(1, ev)
    for p in p_q:
        cm.w_relay(*p)
        start_next()
    cm.ag_relay(1, ev)
    cm.ag_finish(0, xv)
    if g.wide:
        cm.w_finish(*p_small)
        for s in range(g.R):
            r.sm[:, s * 128 : (s + 1) * 128] = r.smalls[s].astype(F32)
        r.fbv[0:1, :] = r.sm[pl.ds(6 + j, 1), :]
    else:
        r.sm[...] = r.small[...].astype(F32)
        r.fbv[0:1, :] = r.fbias[0:1, :]
    nb = 6 + g.FF // D

    outs = []

    def save(src, dst):
        outs.append(cm.local(src, dst, r.os.at[len(outs)]))

    def bias_cols(row):
        return jnp.concatenate([r.sm[row : row + 1, col_block(t)] for t in range(g.NB)], axis=1)

    def row_of(n):
        return r.sm[n : n + 1, :]

    queue = [p_so] + p_c + [p_co] + p_1 + p_2

    def relay(count):
        for _ in range(min(count, len(queue))):
            cm.w_relay(*queue.pop(0))
            start_next()

    plan = list(PLAN)

    zero = jnp.zeros((1, DH), F32)
    for n, v in enumerate((bias_cols(0), zero, bias_cols(1), zero, bias_cols(4), bias_cols(3))):
        r.bias[8 * n : 8 * n + 1, :] = v
    relay(plan[0])
    for p in p_q:
        cm.w_finish(*p)

    def qkv(n):
        r.qkv[n] = (dot(r.x[...], r.wq[n]) + r.bias[pl.ds(n * 8, 1), :]).astype(BF)

    loop(3, qkv)
    relay(plan[1])
    save(r.x, r.o_x)
    save(r.wq, r.o_wq)
    save(r.qkv, r.o_qkv)

    def between_self(a):
        relay(plan[2 + min(a, 1)])

    attend_forward(
        g,
        r.qkv.at[0],
        r.qkv.at[1],
        r.qkv.at[2],
        r.sof.at[j],
        r.pbs,
        g.L,
        True,
        None,
        between_self,
    )
    save(r.pbs, r.o_pbs)
    cm.w_finish(*p_so)
    save(r.wo, r.o_wo)

    buf = types.SimpleNamespace(part=r.part, acc=r.acc, ps=r.ps, pr=r.pr, xs=r.xs, xr=r.xr)

    def projected(src, w):
        def part(xx, dst):
            project(dst, src[at(xx * 2 * Tl, 2 * Tl), :], w)

        return part

    cm.rs_start(0, buf, Tl, projected(r.sof.at[j], r.wo))
    relay(plan[4])
    branch = cm.rs_finish(0, buf) + row_of(2)
    hat, rstd = normalise(xv(j)[...].astype(F32) + branch)
    r.h1[...] = hat
    r.rs1[...] = jnp.broadcast_to(rstd, (Tl, 128))
    first = hat * row_of(nb + 1) + row_of(nb + 4)
    r.res[...] = first
    fv = lambda s: r.fb.at[at(s * Tl, Tl), :]
    r.fb[at(j * Tl, Tl), :] = first.astype(BF)
    cm.ag_start(2, fv)
    save(r.h1, r.o_h1)
    save(r.rs1, r.o_rs1)

    cm.ag_finish(1, ev)
    relay(plan[5])
    for p in p_c:
        cm.w_finish(*p)

    def ckv(n):
        y = dot(r.enc[...], r.wc[n + 1]) + r.bias[pl.ds(n * 8 + 24, 1), :]
        r.ckv[n] = y.astype(BF)

    loop(2, ckv)
    save(r.enc, r.o_enc)
    save(r.ckv, r.o_ckv)
    cm.ag_relay(2, fv)
    save(r.wc, r.o_wc)
    cm.ag_finish(2, fv)
    r.cq[...] = (dot(r.fb[...], r.wc[0]) + r.bias[40:41, :]).astype(BF)
    save(r.fb, r.o_fb)
    save(r.cq, r.o_cq)

    sov = lambda s: r.sof.at[s]
    cov = lambda s: r.cof.at[s]
    cm.ag_start(4, sov)

    relay(plan[6])

    def between_cross(a):
        if a == 0:
            cm.ag_relay(4, sov)
        relay(plan[7 + min(a, 1)])

    attend_forward(
        g,
        r.cq,
        r.ckv.at[0],
        r.ckv.at[1],
        r.cof.at[j],
        r.pbc,
        g.E,
        False,
        r.lens[1],
        between_cross,
    )
    save(r.pbc, r.o_pbc)
    cm.w_finish(*p_co)
    save(r.wd, r.o_wd)
    cm.rs_start(1, buf, Tl, projected(r.cof.at[j], r.wd))
    relay(plan[9])
    branch = cm.rs_finish(1, buf) + row_of(5)
    hat, rstd = normalise(r.res[...] + branch)
    r.h2[...] = hat
    r.rs2[...] = jnp.broadcast_to(rstd, (Tl, 128))
    second = hat * row_of(nb + 2) + row_of(nb + 5)
    r.res[...] = second
    sv = lambda s: r.sb.at[at(s * Tl, Tl), :]
    r.sb[at(j * Tl, Tl), :] = second.astype(BF)
    cm.ag_start(3, sv)
    save(r.h2, r.o_h2)
    save(r.rs2, r.o_rs2)

    relay(plan[10])
    cm.ag_relay(3, sv)
    relay(plan[11])
    cm.ag_finish(3, sv)
    cm.ag_start(5, cov)
    cm.ag_finish(4, sov)
    save(r.sof, r.o_sof)
    while len(queue) > n2 or staged:
        relay(1)
    done = n2 - len(queue)
    first1, first2 = p_1[0][0], p_2[0][0]

    def piece1(n):
        return first1 + n, lambda s: r.w1.at[at(s * Dl, Dl), at(n * 256, 256)]

    def piece2(n):
        return first2 + n, lambda s: r.w2.at[at(s * FB, FB), at(n * 256, 256)]

    for p in queue[: len(queue) % n1]:
        cm.w_relay(*p)
        done += 1
    each = (n2 - done) // n1

    def hidden(n):
        cm.w_finish(*piece1(n))
        cols = at(n * 256, 256)
        pre = dot(r.sb[...], r.w1[:, cols]) + r.fbv[0:1, cols]
        cdf = 0.5 * (1.0 + lax.erf(pre * 0.7071067811865476))
        r.hid[:, cols] = (pre * cdf).astype(BF)
        r.dg[:, cols] = (cdf + pre * jnp.exp(-0.5 * pre * pre) * 0.3989422804014327).astype(BF)
        for e in range(each):
            cm.w_relay(*piece2(done + n * each + e))

    loop(n1, hidden)
    cm.ag_relay(5, cov)
    save(r.sb, r.o_sb)
    save(r.w1, r.o_w1)
    save(r.hid, r.o_hid)
    save(r.dg, r.o_dg)
    for p in p_2:
        cm.w_finish(*p)
    save(r.w2, r.o_w2)
    cm.rs_start(2, buf, Tl, projected(r.hid, r.w2))
    cm.ag_finish(5, cov)
    save(r.cof, r.o_cof)
    branch = cm.rs_finish(2, buf) + row_of(nb)
    hat, rstd = normalise(r.res[...] + branch)
    r.h3[...] = hat
    r.rs3[...] = jnp.broadcast_to(rstd, (Tl, 128))
    third = hat * row_of(nb + 3) + row_of(nb + 6)
    row = j * Tl + lax.broadcasted_iota(jnp.int32, (Tl, 1), 0)
    live = (row < r.lens[0]).astype(F32)
    r.lo[...] = (third * live).astype(BF)
    save(r.h3, r.o_h3)
    save(r.rs3, r.o_rs3)
    save(r.lo, r.o_lo)
    save(r.sm, r.o_sm)

    for p in pieces:
        cm.w_drain(*p)
    for k, v in enumerate((xv, ev, fv, sv, sov, cov)):
        cm.ag_drain(k, v)
    for d in outs:
        d.wait()


def forward_call(g, ins):
    names, in_specs, args = [], [], []
    for n, a in ins.items():
        names.append(n)
        args.append(a)
        if n == LENS:
            in_specs.append(pl.BlockSpec(memory_space=pltpu.SMEM))
        elif a.size <= 8 * FJ_MAX and n != LENS:
            in_specs.append(pl.BlockSpec(memory_space=pltpu.VMEM))
        else:
            in_specs.append(ANY)
    D, L, E, Tl = g.D, g.L, g.E, g.Tl
    keep = dict(
        x=((L, D), BF),
        enc=((E, D), BF),
        wq=((3, D, g.DH), BF),
        wo=((g.DH, D), BF),
        wc=((3, D, g.DH), BF),
        wd=((g.DH, D), BF),
        w1=((D, g.FJ), BF),
        w2=((g.FJ, D), BF),
        sm=((NS, D), F32),
        qkv=((3, L, g.DH), BF),
        sof=((g.S, L, g.DH), BF),
        pbs=((g.H, L, L), BF),
        fb=((L, D), BF),
        cq=((L, g.DH), BF),
        ckv=((2, E, g.DH), BF),
        cof=((g.S, L, g.DH), BF),
        pbc=((g.H, L, E), BF),
        sb=((L, D), BF),
        hid=((L, g.FJ), BF),
        dg=((L, g.FJ), BF),
        h1=((Tl, D), F32),
        h2=((Tl, D), F32),
        h3=((Tl, D), F32),
        rs1=((Tl, 128), F32),
        rs2=((Tl, 128), F32),
        rs3=((Tl, 128), F32),
        lo=((Tl, D), BF),
    )
    out_shape = [jax.ShapeDtypeStruct(*s) for s in keep.values()]
    names += ["o_" + n for n in keep]
    scratch = {n: pltpu.VMEM(*s) for n, s in keep.items()}
    scratch.update(res=pltpu.VMEM((Tl, D), F32))
    scratch.update(part=pltpu.VMEM((2 * Tl, D), F32))
    scratch.update(acc=pltpu.VMEM((g.X, Tl, D), F32))
    two = pltpu.VMEM((g.X, Tl, D), BF)
    one = pltpu.VMEM((g.X - 1, Tl, D), BF)
    scratch.update(ps=two, pr=two, xs=one, xr=one)
    if g.wide:
        scratch.update(smalls=pltpu.VMEM((g.R, NS, 128), BF), mine=pltpu.VMEM((NS, 128), F32))
    scratch.update(bias=pltpu.VMEM((48, g.DH), F32), fbv=pltpu.VMEM((8, g.FJ), F32))
    sem = pltpu.SemaphoreType.DMA
    NP = 9 + g.FJ // 256 + D // 256
    scratch.update(ls=sem((6,)))
    scratch.update(lq=sem((g.NB,)))
    scratch.update(lc=sem((g.NB,)))
    scratch.update(l1=sem((g.R,)))
    scratch.update(os=sem((len(keep),)))
    scratch.update(wzs=sem((NP, g.Z - 1)))
    scratch.update(wzr=sem((NP, g.Z - 1)))
    scratch.update(wys=sem((NP, g.Y - 1, g.Z)))
    scratch.update(wyr=sem((NP, g.Y - 1, g.Z)))
    scratch.update(axs=sem((6, g.X - 1)))
    scratch.update(axr=sem((6, g.X - 1)))
    scratch.update(acs=sem((6, g.X)))
    scratch.update(acr=sem((6, g.X)))
    scratch.update(rcs=sem((3, g.X)))
    scratch.update(rcr=sem((3, g.X)))
    scratch.update(rxs=sem((3, g.X - 1)))
    scratch.update(rxr=sem((3, g.X - 1)))
    names += list(scratch)
    out = pl.pallas_call(
        functools.partial(forward_kernel, g, names),
        out_shape=out_shape,
        in_specs=in_specs,
        out_specs=[ANY] * len(out_shape),
        scratch_shapes=list(scratch.values()),
        compiler_params=pltpu.CompilerParams(
            collective_id=0, has_side_effects=True, vmem_limit_bytes=60 << 20
        ),
    )(*args)
    return dict(zip(keep, out))


def attend_backward(g, q_ref, k_ref, v_ref, do_ref, src, bufs, outs, acc, Lk, causal, between):
    lane = lax.broadcasted_iota(jnp.int32, (1, 128), 1)
    low = lane < HD
    scale = HD ** -0.5
    dq_ref, dk_ref, dv_ref = outs
    dka, dva = acc
    pbuf, psem = bufs
    top = g.L // CH - 1

    def width(a):
        return (a + 1) * CH if causal else Lk

    def fetch(t, a, e):
        kk = width(a)
        return pltpu.make_async_copy(
            src.at[2 * t + e, pl.ds(a * CH, CH), pl.ds(0, kk)],
            pbuf.at[e, :, pl.ds(0, kk)],
            psem.at[e],
        )

    fetch(0, top, 0).start()
    for a in range(top, -1, -1):
        rows = pl.ds(a * CH, CH)
        kk = width(a)
        keys = pl.ds(0, kk)

        def body(t):
            cols = at(t * 128, 128)
            q = q_ref[rows, cols]
            do = do_ref[rows, cols]
            k = k_ref[keys, cols]
            v = v_ref[keys, cols]
            zero = jnp.zeros_like(q)
            dqs = []
            for e in range(2):
                fetch(t, a, e).wait()
                if e == 0:
                    fetch(t, a, 1).start()
                else:

                    @pl.when(t + 1 < g.NB)
                    def _():
                        fetch(t + 1, a, 0).start()

                    if a:

                        @pl.when(t + 1 == g.NB)
                        def _():
                            fetch(0, a - 1, 0).start()

                mine = low if e == 0 else ~low
                qe = jnp.where(mine, q, zero)
                doe = jnp.where(mine, do, zero)
                p = pbuf[e, :, keys]
                pf = p.astype(F32)
                w = dot_nt(doe, v) * pf
                ds = (w - pf * jnp.sum(w, axis=-1, keepdims=True)).astype(BF)
                dqs.append(dot(ds, k))
                dk = dot_tn(ds, qe)
                dv = dot_tn(p, doe)
                if a == top and e == 0:
                    dka[t, keys, :] = dk
                    dva[t, keys, :] = dv
                else:
                    dka[t, keys, :] += dk
                    dva[t, keys, :] += dv
            dq_ref[rows, cols] = (jnp.where(low, dqs[0], dqs[1]) * scale).astype(BF)

        loop(g.NB, body)
        between(a)

    def finish(t):
        cols = at(t * 128, 128)
        keys = pl.ds(0, Lk)
        dk_ref[keys, cols] = (dka[t, keys, :] * scale).astype(BF)
        dv_ref[keys, cols] = dva[t, keys, :].astype(BF)

    loop(g.NB, finish)


class Rows:
    def __init__(self, ref, first, size):
        self.ref, self.first, self.size, self.dtype = ref, first, size, ref.dtype
        self.at = self

    def rows(self, d):
        return pl.ds((self.first + d) * self.size, self.size)

    def __getitem__(self, d):
        return self.ref.at[self.rows(d), :]

    def __setitem__(self, d, value):
        self.ref[self.rows(d), :] = value


def colsum(v):
    return jnp.sum(v.astype(F32), axis=0, keepdims=True)


def backward_kernel(g, names, *refs):
    r = types.SimpleNamespace(**dict(zip(names, refs)))
    cm = Comm(g, r)
    i, j, c = cm.i, cm.j, cm.c
    Tl, El, D, Dl, DH, FB, FJ = g.Tl, g.El, g.D, g.Dl, g.DH, g.FB, g.FJ
    nb = 6 + g.FF // D

    loads = []

    def load(src, dst):
        loads.append(cm.local(src, dst, r.ls.at[len(loads)]))
        return loads[-1]

    l_og = load(r.i_og, r.og)
    l_h3 = load(r.i_h3, r.h3)
    l_rs3 = load(r.i_rs3, r.rs3)
    l_sm = load(r.i_sm, r.sm)
    l_w2 = load(r.i_w2, r.w2)
    l_dg = load(r.i_dg, r.dg)
    l_w1 = load(r.i_w1, r.w1)
    l_hid = load(r.i_hid, r.hid)
    l_sb = load(r.i_sb, r.sb)
    l_h2 = load(r.i_h2, r.h2)
    l_rs2 = load(r.i_rs2, r.rs2)
    l_wd = load(r.i_wd, r.wd)
    l_cof = load(r.i_cof, r.cof)
    l_ckv = load(r.i_ckv, r.ckv)
    l_cq = load(r.i_cq, r.cq)
    l_wc = load(r.i_wc, r.wc)
    l_fb = load(r.i_fb, r.fb)
    l_enc = load(r.i_enc, r.enc)
    l_h1 = load(r.i_h1, r.h1)
    l_rs1 = load(r.i_rs1, r.rs1)
    l_wo = load(r.i_wo, r.wo)
    l_qkv = load(r.i_qkv, r.qkv)
    l_sof = load(r.i_sof, r.sof)
    l_wq = load(r.i_wq, r.wq)

    cm.barrier()
    r.sg[...] = jnp.zeros_like(r.sg)

    def col_block(t):
        return pl.ds(pl.multiple_of((t * g.S + j) * 128, 128), 128)

    def put_cols(row, value):
        for t in range(g.NB):
            r.sg[row : row + 1, col_block(t)] = value[:, t * 128 : (t + 1) * 128]

    own = at(j * Tl, Tl)

    def norm_back(gr, hat, rstd, n):
        r.sg[nb + 1 + n : nb + 2 + n, :] = jnp.sum(gr * hat, axis=0, keepdims=True)
        r.sg[nb + 4 + n : nb + 5 + n, :] = jnp.sum(gr, axis=0, keepdims=True)
        gn = gr * r.sm[nb + 1 + n : nb + 2 + n, :]
        return rstd[:, 0:1] * (
            gn
            - jnp.mean(gn, axis=-1, keepdims=True)
            - hat * jnp.mean(gn * hat, axis=-1, keepdims=True)
        )

    def send_dy(k, dh, buf, bias_row):
        low = dh.astype(BF)
        buf[own, :] = low
        view = lambda s: buf.at[at(s * Tl, Tl), :]
        cm.ag_start(k, view)
        r.sg[bias_row : bias_row + 1, :] = colsum(low)
        return view

    n1 = FJ // 256
    n2 = D // 256
    tasks = []

    def task(view, yr, zr, out):
        tasks.append((len(tasks), view, yr, zr, out))
        return tasks[-1]

    t_2 = [
        task(
            lambda s, n=n: r.d2.at[at(s * FB, FB), pl.ds(n * 256, 256)],
            r.yr2.at[n],
            r.zr2.at[n],
            r.g2.at[j, :, pl.ds(n * 256, 256)],
        )
        for n in range(n2)
    ]
    t_1 = [
        task(
            lambda s, n=n: r.d1.at[at(s * Dl, Dl), pl.ds(n * 256, 256)],
            r.yr1.at[n],
            r.zr1.at[n],
            r.g1.at[j, :, pl.ds(n * 256, 256)],
        )
        for n in range(n1)
    ]
    t_c = [
        task(
            lambda s, n=n: r.dc.at[n, at(s * Dl, Dl), :], r.yrc.at[n], r.zrc.at[n], r.gc.at[j, n]
        )
        for n in range(4)
    ]
    t_s = [
        task(
            lambda s, n=n: r.ds.at[n, at(s * Dl, Dl), :], r.yrs.at[n], r.zrs.at[n], r.gs.at[j, n]
        )
        for n in range(4)
    ]
    if g.wide:
        t_g = task(
            lambda s: r.sg.at[:, pl.ds(pl.multiple_of(s * 128, 128), 128)],
            r.yrg,
            r.zrg,
            r.gg.at[j],
        )
    waiting, turns, ends = [], [], []

    def pump():
        while waiting and len(turns) < AHEAD_Y:
            t = waiting.pop(0)
            cm.g_start(t)
            turns.append(t)

    def launch(*ts):
        waiting.extend(ts)
        pump()

    def turn(count):
        for _ in range(min(count, len(turns) + len(waiting))):
            t = turns.pop(0)
            cm.g_turn(t)
            ends.append(t)
            pump()

    def complete(group):
        for t in group:
            while t not in ends:
                turn(1)
            cm.g_finish(t)
            ends.remove(t)

    points = list(BPLAN)

    def point():
        turn(points.pop(0) if points else 0)

    outs = []
    outs2 = []
    finals = []

    def save(src, dst):
        outs.append(cm.local(src, dst, r.os.at[len(outs)]))

    def save_2(s):
        return [(r.g2.at[s], r.o_f2.at[at(s * FB, FB), :])]

    def save_1(s):
        if not g.wide:
            return [(r.g1.at[s], r.o_f1.at[s])]
        return [
            (r.g1.at[s, :, pl.ds(t * 128, 128)], r.o_f1.at[:, at((t * g.S + s) * 128, 128)])
            for t in range(g.R)
        ]

    def save_n(src, d3, d1, parts=range(4)):
        def pairs(s):
            res = []
            for t in range(g.NB):
                cols = at((t * g.S + s) * 128, 128)
                mine = pl.ds(t * 128, 128)
                for n in parts:
                    dst = d3.at[n, :, cols] if n < 3 else d1.at[:, cols]
                    res.append((src.at[s, n, :, mine], dst))
            return res

        return pairs

    def gather(k, view, pairs):
        cm.ag_start(k, view)
        finals.append((k, view, pairs))

    def flush():
        for k, view, pairs in finals:
            cm.ag_finish(k, view)
            todo = [pair for s in range(g.S) for pair in pairs(s)]
            for n, (src, dst) in enumerate(todo):
                outs2.append(cm.local(src, dst, r.fs.at[k - 3, n]))

    for d in (l_og, l_h3, l_rs3, l_sm):
        d.wait()
    row = j * Tl + lax.broadcasted_iota(jnp.int32, (Tl, 1), 0)
    live = (row < r.lens[0]).astype(F32)
    g3 = r.og[...].astype(F32) * live
    dh3 = norm_back(g3, r.h3[...], r.rs3[...], 2)
    r.dh[...] = dh3
    v3 = send_dy(0, dh3, r.dya, nb)

    for d in (l_w2, l_dg, l_hid):
        d.wait()
    cm.ag_relay(0, v3)
    cm.ag_finish(0, v3)

    def grad_2(n):
        cols = at(n * 256, 256)
        r.d2[:, cols] = dot_tn(r.hid[...], r.dya[:, cols]).astype(BF)

    def hidden_back(n):
        cols = at(n * 256, 256)
        y = dot_nt(r.dya[...], r.w2[cols, :]) * r.dg[:, cols].astype(F32)
        y = y.astype(BF)
        r.dpre[:, cols] = y
        r.fsum[0:1, cols] = colsum(y)

    grad_2(0)
    launch(t_2[0])
    loop(n2 - 1, lambda n: grad_2(n + 1))
    launch(*t_2[1:])
    loop(n1, hidden_back)
    point()
    if g.wide:
        r.sg[pl.ds(6 + j, 1), :] = r.fsum[0:1, :]
    else:
        r.fg[...] = r.fsum[...]
    l_w1.wait()

    def part3(xx, dst):
        project(dst, r.dpre[at(xx * 2 * Tl, 2 * Tl), :], r.w1, True)

    buf = types.SimpleNamespace(part=r.part, acc=r.acc, ps=r.ps, pr=r.pr, xs=r.xs, xr=r.xr)
    cm.rs_start(0, buf, Tl, part3)
    l_sb.wait()
    point()

    def grad_1(n):
        cols = at(n * 256, 256)
        r.d1[:, cols] = dot_tn(r.sb[...], r.dpre[:, cols]).astype(BF)

    loop(n1, grad_1)
    l_x = load(r.i_x, r.sb)
    launch(*t_1)
    for d in (l_h2, l_rs2):
        d.wait()
    point()
    dh2 = norm_back(r.dh[...] + cm.rs_finish(0, buf), r.h2[...], r.rs2[...], 1)
    r.dh[...] = dh2
    v2 = send_dy(1, dh2, r.dyb, 5)
    for d in (l_wd, l_ckv, l_cq):
        d.wait()
    point()
    cm.ag_relay(1, v2)
    point()

    cm.ag_finish(1, v2)
    r.do[...] = dot_nt(r.dyb[...], r.wd[...]).astype(BF)
    point()

    def between_cross(a):
        point()

    attend_backward(
        g,
        r.cq,
        r.ckv.at[0],
        r.ckv.at[1],
        r.do,
        r.i_pbc,
        (r.pbuf, r.psem),
        (r.dcq, r.dckv.at[0], r.dckv.at[1]),
        (r.dka, r.dva),
        g.E,
        False,
        between_cross,
    )
    l_wc.wait()

    def part4(xx, dst):
        project(dst, r.dcq[at(xx * 2 * Tl, 2 * Tl), :], r.wc.at[0], True)

    cm.ag_drain(0, v3)
    cm.rs_start(1, buf, Tl, part4)
    point()
    put_cols(3, colsum(r.dcq[...]))
    put_cols(4, colsum(r.dckv[1]))
    for d in (l_fb, l_h1, l_rs1, l_enc):
        d.wait()

    def grad_rows(dst, a, b):
        def body(n):
            rows = at(n * 256, 256)
            dst[rows, :] = dot_tn(a[:, rows], b[...]).astype(BF)

        loop(D // 256, body)

    grad_rows(r.dc.at[1], r.enc, r.dckv.at[0])
    launch(t_c[1])
    point()
    dh1 = norm_back(r.dh[...] + cm.rs_finish(1, buf), r.h1[...], r.rs1[...], 0)
    r.dh[...] = dh1
    v1 = send_dy(2, dh1, r.dya, 2)
    point()
    grad_rows(r.dc.at[2], r.enc, r.dckv.at[1])
    launch(t_c[2])
    point()
    cm.ag_relay(2, v1)
    grad_rows(r.dc.at[0], r.fb, r.dcq)
    launch(t_c[0])
    point()
    complete(t_2)
    gather(3, lambda s: r.g2.at[s], save_2)
    ebuf = types.SimpleNamespace(
        acc=Rows(r.enc, 0, El), ps=Rows(r.enc, g.X, El), pr=r.epr, xs=r.exs, xr=r.exr
    )

    def part_e(rows):
        return dot_nt(r.dckv[0, rows, :], r.wc[1]) + dot_nt(r.dckv[1, rows, :], r.wc[2])

    def grad_out(full, dy, dst):
        dyj = jnp.concatenate([dy[:, col_block(t)] for t in range(g.NB)], axis=1)

        def body(s):
            y = dot_tn(full[s], dyj).astype(BF)
            for t in range(g.NB):
                dst[at((t * g.S + s) * 128, 128), :] = y[t * 128 : (t + 1) * 128, :]

        loop(g.S, body)

    for d in (l_wo, l_qkv, l_cof, l_sof):
        d.wait()
    grad_out(r.cof, r.dyb, r.dc.at[3])
    launch(t_c[3])
    point()

    cm.ag_finish(2, v1)
    r.do[...] = dot_nt(r.dya[...], r.wo[...]).astype(BF)
    grad_out(r.sof, r.dya, r.ds.at[3])
    launch(t_s[3])
    point()
    cm.rs_start_halves(3, ebuf, El, part_e)
    complete(t_1)
    gather(4, lambda s: r.g1.at[s], save_1)

    def between_self(a):
        if a == g.L // CH - 1:
            cm.ag_relay(*finals[0][:2])
            cm.rs_turn(3, ebuf)
        point()

    attend_backward(
        g,
        r.qkv.at[0],
        r.qkv.at[1],
        r.qkv.at[2],
        r.do,
        r.i_pbs,
        (r.pbuf, r.psem),
        (r.dqkv.at[0], r.dqkv.at[1], r.dqkv.at[2]),
        (r.dka, r.dva),
        g.L,
        True,
        between_self,
    )
    for d in (l_wq, l_x):
        d.wait()

    def part5(xx, dst):
        rows = at(xx * 2 * Tl, 2 * Tl)

        def body(n):
            cols = at(n * 256, 256)
            dst[:, cols] = (
                dot_nt(r.dqkv[0, rows, :], r.wq[0, cols, :])
                + dot_nt(r.dqkv[1, rows, :], r.wq[1, cols, :])
                + dot_nt(r.dqkv[2, rows, :], r.wq[2, cols, :])
            )

        loop(D // 256, body)

    put_cols(0, colsum(r.dqkv[0]))
    put_cols(1, colsum(r.dqkv[2]))
    if g.wide:
        launch(t_g)
    for n in range(3):
        grad_rows(r.ds.at[n], r.sb, r.dqkv.at[n])
        launch(t_s[n])
        point()
    cm.rs_start(2, buf, Tl, part5)
    cm.ag_relay(*finals[1][:2])
    complete(t_c)
    gather(5, lambda s: r.gc.at[s], save_n(r.gc, r.o_cq, r.o_co))
    r.ge[...] = cm.rs_finish(3, ebuf).astype(BF)
    save(r.ge, r.o_ge)
    r.gi[...] = (r.dh[...] + cm.rs_finish(2, buf)).astype(BF)
    save(r.gi, r.o_gi)
    order = [3, 0, 1, 2]
    for m, n in enumerate(order):
        complete([t_s[n]])
        gather(6 + n, lambda s, n=n: r.gs.at[s, n], save_n(r.gs, r.o_sq, r.o_so, [n]))
        cm.ag_relay(*finals[m + 2][:2])
        if n == 3 and g.wide:
            complete([t_g])
            cm.ag_start(10, lambda s: r.gg.at[s])
    cm.ag_relay(*finals[6][:2])
    v_gg = lambda s: r.gg.at[s]
    if g.wide:
        cm.ag_relay(10, v_gg)
        cm.ag_finish(10, v_gg)
    flush()
    if g.wide:
        total = r.gg[0]
        for s in range(1, g.S):
            total = total + r.gg[s]
        r.gsum[...] = total
        save(r.gsum, r.o_small)
    else:
        save(r.sg, r.o_small)
        save(r.fg, r.o_fg)

    cm.ag_drain(1, v2)
    cm.ag_drain(2, v1)
    for k, view, pairs in finals:
        cm.ag_drain(k, view)
    if g.wide:
        cm.ag_drain(10, v_gg)
    for t in tasks:
        cm.g_drain(t)
    for d in outs + outs2:
        d.wait()


def backward_call(g, lens, out_grad, f):
    D, L, E, Tl, El, S = g.D, g.L, g.E, g.Tl, g.El, g.S
    Dl, DH, FJ, FB = g.Dl, g.DH, g.FJ, g.FB
    loaded = [n for n in f if n not in PROBS and n != FIRST]
    names = ["lens", "i_og"] + ["i_" + n for n in f]
    args = [lens, out_grad] + list(f.values())
    in_specs = [pl.BlockSpec(memory_space=pltpu.SMEM)] + [ANY] * (len(args) - 1)
    V = pltpu.VMEM
    scratch = {n: V(f[n].shape, f[n].dtype) for n in loaded}
    small = (NS, 128) if g.wide else (NS, D)
    outs = dict(
        gi=((Tl, D), BF),
        ge=((El, D), BF),
        f2=((g.FR, D), BF),
        f1=((Dl, g.FF) if g.wide else (S, Dl, FJ), BF),
        cq=((3, Dl, D), BF),
        co=((Dl, D), BF),
        sq=((3, Dl, D), BF),
        so=((Dl, D), BF),
        small=(small, F32),
    )
    if not g.wide:
        outs.update(fg=((8, FJ), F32))
        scratch.update(fg=V((8, FJ), F32))
    names += ["o_" + n for n in outs]
    scratch.update(
        gi=V((Tl, D), BF),
        ge=V((El, D), BF),
        g2=V((S, FB, D), BF),
        g1=V((S, Dl, FJ), BF),
        gc=V((S, 4, Dl, DH), BF),
        gs=V((S, 4, Dl, DH), BF),
        fsum=V((8, FJ), F32),
    )
    two = V((g.X, Tl, D), BF)
    one = V((g.X - 1, Tl, D), BF)
    scratch.update(
        og=V((Tl, D), BF),
        dh=V((Tl, D), F32),
        sg=V((NS, D), F32),
        part=V((2 * Tl, D), F32),
        acc=V((g.X, Tl, D), F32),
        ps=two,
        pr=two,
        xs=one,
        xr=one,
        epr=V((g.X, El, D), BF),
        exs=V((g.X - 1, El, D), BF),
        exr=V((g.X - 1, El, D), BF),
        dya=V((L, D), BF),
        dyb=V((L, D), BF),
        dpre=V((L, FJ), BF),
        do=V((L, DH), BF),
        dcq=V((L, DH), BF),
        dckv=V((2, E, DH), BF),
        dqkv=V((3, L, DH), BF),
        dka=V((g.NB, E, 128), F32),
        dva=V((g.NB, E, 128), F32),
        pbuf=V((2, CH, E), BF),
        d2=V((FJ, D), BF),
        d1=V((D, FJ), BF),
        dc=V((4, D, DH), BF),
        ds=V((4, D, DH), BF),
        yr2=V((D // 256, g.Y - 1, g.Z, FB, 256), BF),
        yr1=V((FJ // 256, g.Y - 1, g.Z, Dl, 256), BF),
        yrc=V((4, g.Y - 1, g.Z, Dl, DH), BF),
        yrs=V((4, g.Y - 1, g.Z, Dl, DH), BF),
        zr2=V((D // 256, g.Z - 1, FB, 256), BF),
        zr1=V((FJ // 256, g.Z - 1, Dl, 256), BF),
        zrc=V((4, g.Z - 1, Dl, DH), BF),
        zrs=V((4, g.Z - 1, Dl, DH), BF),
    )
    if g.wide:
        scratch.update(
            yrg=V((g.Y - 1, g.Z, NS, 128), F32),
            zrg=V((g.Z - 1, NS, 128), F32),
            gg=V((S, NS, 128), F32),
            gsum=V((NS, 128), F32),
        )
    sem = pltpu.SemaphoreType.DMA
    NP = 9 + FJ // 256 + D // 256
    scratch.update(
        ls=sem((26,)),
        os=sem((8,)),
        psem=sem((2,)),
        fs=sem((7, max(S * (g.R if g.wide else 1), 4 * S * g.NB))),
        gys=sem((NP, g.Y - 1, g.Z)),
        gyr=sem((NP, g.Y - 1, g.Z)),
        gzs=sem((NP, g.Z - 1)),
        gzr=sem((NP, g.Z - 1)),
        axs=sem((11, g.X - 1)),
        axr=sem((11, g.X - 1)),
        acs=sem((11, g.X)),
        acr=sem((11, g.X)),
        rcs=sem((4, g.X)),
        rcr=sem((4, g.X)),
        rxs=sem((4, g.X - 1)),
        rxr=sem((4, g.X - 1)),
    )
    names += list(scratch)
    out = pl.pallas_call(
        functools.partial(backward_kernel, g, names),
        out_shape=[jax.ShapeDtypeStruct(*s) for s in outs.values()],
        in_specs=in_specs,
        out_specs=[ANY] * len(outs),
        scratch_shapes=list(scratch.values()),
        compiler_params=pltpu.CompilerParams(
            collective_id=1, has_side_effects=True, vmem_limit_bytes=67043328
        ),
    )(*args)
    return dict(zip(outs, out))


def finish_kernel(cuts, *refs):
    half = (len(refs) - len(cuts)) // 2
    ins, small = refs[:half], refs[half]
    outs, smalls = refs[half + 1 : 2 * half + 1], refs[2 * half + 1 :]
    for src, dst in zip(ins, outs):
        dst[...] = src[...].astype(dst.dtype)
    for (lo, hi), dst in zip(cuts, smalls):
        dst[...] = small[lo:hi, :]


def finish_call(g, parts, small):
    steps = 4 if g.Dl % 64 == 0 else 2
    nf = g.FF // g.D
    cuts = ((0, 6), (6, 6 + nf), (6 + nf, 7 + nf), (7 + nf, 10 + nf), (10 + nf, 13 + nf))
    specs, shapes = [], []
    for n, (a, dtype) in enumerate(parts):
        block = list(a.shape)
        block[-2] //= steps
        lead = a.ndim - 2
        specs.append(pl.BlockSpec(tuple(block), lambda k, lead=lead: (0,) * lead + (k, 0)))
        shapes.append(jax.ShapeDtypeStruct(a.shape, dtype))
    for lo, hi in cuts:
        shapes.append(jax.ShapeDtypeStruct((hi - lo, small.shape[1]), F32))

    def whole(shape):
        return pl.BlockSpec(shape, lambda k: (0, 0))

    return pl.pallas_call(
        functools.partial(finish_kernel, cuts),
        grid=(steps,),
        out_shape=shapes,
        in_specs=specs + [whole(small.shape)],
        out_specs=specs + [whole(s.shape) for s in shapes[len(specs) :]],
        compiler_params=pltpu.CompilerParams(vmem_limit_bytes=67043328),
    )(*[a for a, _ in parts], small)


def on_device(
    decoder_in,
    encoder_states,
    out_grad,
    seq_lengths,
    enc_lengths,
    self_qkv,
    self_out,
    cross_qkv,
    cross_out,
    attn_bias,
    ffn_in,
    ffn_in_bias,
    ffn_out,
    ffn_out_bias,
    norm_gain,
    norm_bias,
):
    R = lax.axis_size(DP)
    S = lax.axis_size(SEQ)
    j = lax.axis_index(SEQ)
    D = decoder_in.shape[2]
    FF = ffn_in.shape[1]
    g = configure(R, S, decoder_in.shape[1], encoder_states.shape[1], D, FF)
    Dl, FR, FB, FJ, NB = g.Dl, g.FR, g.FB, g.FJ, g.NB
    nf = FF // D
    nb = 6 + nf

    fi, fo = ffn_in_bias.reshape(nf, Dl), ffn_out_bias.reshape(1, Dl)
    lens = jnp.concatenate([seq_lengths, enc_lengths])
    ins = dict(
        lens=lens,
        tok=decoder_in[0],
        states=encoder_states[0],
        self_qkv=self_qkv,
        self_out=self_out,
        cross_qkv=cross_qkv,
        cross_out=cross_out,
        ffn_in=ffn_in,
        ffn_out=ffn_out,
    )
    if g.wide:
        ins.update(
            attn_bias=attn_bias,
            ffn_in_bias=fi,
            ffn_out_bias=fo,
            norm_gain=norm_gain,
            norm_bias=norm_bias,
        )
    else:
        pad = jnp.zeros((NS - nb - 7, Dl), BF)
        small = jnp.concatenate([attn_bias, fi, fo, norm_gain, norm_bias, pad])
        small = lax.all_gather(small, DP, axis=1, tiled=True)
        fb = small[6:nb].reshape(nf, R, Dl).transpose(1, 0, 2)
        fb = lax.dynamic_slice_in_dim(fb.reshape(R, FR), j * FB, FB, axis=1).reshape(1, -1)
        packed = lax.dynamic_slice_in_dim(ffn_in.reshape(Dl, R, FR), j * FB, FB, axis=2)
        ins.update(
            small=small,
            fbias=jnp.broadcast_to(fb.astype(F32), (8, FJ)),
            ffn_in=packed.reshape(Dl, FJ),
        )
    f = forward_call(g, ins)
    lo = f.pop(LO)
    b = types.SimpleNamespace(**backward_call(g, lens, out_grad[0], f))

    sm = b.small
    if not g.wide:
        fpl = lax.dynamic_update_slice(
            jnp.zeros((R, S, FB), F32), b.fg[0].reshape(R, 1, FB), (0, j, 0)
        )
        fpl = fpl.reshape(R, nf, Dl).transpose(1, 0, 2).reshape(nf, D)
        sm = lax.dynamic_update_slice(sm, fpl, (6, 0))
        sm = lax.psum(lax.psum_scatter(sm, DP, scatter_dimension=1, tiled=True), SEQ)

    gw1 = b.f1
    if not g.wide:
        gw1 = gw1.reshape(S, Dl, R, FB).transpose(1, 2, 0, 3).reshape(Dl, FF)
    parts = [(lo, BF), (b.gi, BF), (b.ge, BF)]
    parts += [(a, F32) for a in (b.sq, b.so, b.cq, b.co, gw1, b.f2)]
    lo, gi, ge, sq, so, cq, co, f1, f2, gab, gfi, gfo, ggain, gshift = finish_call(g, parts, sm)
    return (
        lo[None],
        gi[None],
        ge[None],
        sq,
        so,
        cq,
        co,
        gab,
        f1,
        gfi.reshape(-1),
        f2,
        gfo.reshape(-1),
        ggain,
        gshift,
    )


def solution(mesh):
    act = P(DP, SEQ, None)
    w3 = P(None, DP, None)
    w2 = P(DP, None)
    v2 = P(None, DP)
    v1 = P(DP)
    return jax.shard_map(
        on_device,
        mesh=mesh,
        in_specs=(act, act, act, v1, v1, w3, w2, w3, w2, v2, w2, v1, w2, v1, v2, v2),
        out_specs=(act, act, act, w3, w2, w3, w2, v2, w2, v1, w2, v1, v2, v2),
        check_vma=False,
    )
```

```python
import functools
import types

import jax
import jax.numpy as jnp
from jax import lax
from jax.experimental import pallas as pl
from jax.experimental.pallas import tpu as pltpu
from jax.sharding import PartitionSpec as P

HD = 64
EPS = 1e-05
F32 = jnp.float32
BF = jnp.bfloat16
MESH = pl.DeviceIdType.MESH
ANY = pl.BlockSpec(memory_space=pl.ANY)
CH = 256
NS = 32
DP = "dp"
SEQ = "seq"
LENS = "lens"
FJ_MAX = 4096
AHEAD = 2
AHEAD_Y = 2
PLAN = (1, 1, 1, 1, 2, 1, 1, 1, 1, 1, 1, 0, 1)
BPLAN = (0, 1, 1, 1, 0, 1, 2, 1, 1, 0, 1, 0, 1, 0, 1, 1, 1, 0, 1, 1)


def configure(R, S, Tl, El, D, FF):
    g = types.SimpleNamespace(R=R, S=S, Tl=Tl, El=El, D=D, FF=FF)
    g.Y = 1
    while 8 * g.Y * g.Y <= R:
        g.Y *= 2
    g.Z = R // g.Y
    g.X = S // 2
    g.Dl = D // R
    g.FR = FF // R
    g.FB = g.FR // S
    g.DH = D // S
    g.FJ = FF // S
    g.NB = g.DH // 128
    g.H = g.DH // HD
    g.L = Tl * S
    g.E = El * S
    g.wide = g.Dl == 128 and g.FB == 128
    return g


def dot(a, b):
    return jnp.dot(a, b, preferred_element_type=F32)


def dot_nt(a, b):
    return lax.dot_general(a, b, (((1,), (1,)), ((), ())), preferred_element_type=F32)


def dot_tn(a, b):
    return lax.dot_general(a, b, (((0,), (0,)), ((), ())), preferred_element_type=F32)


def rem(a, b):
    return lax.rem(a, jnp.int32(b))


def at(start, size):
    if isinstance(start, int):
        return pl.ds(start, size)
    return pl.ds(pl.multiple_of(start, size), size)


def loop(count, body):
    if count == 1:
        body(0)
    else:
        lax.fori_loop(0, count, lambda n, z: (body(n), z)[1], 0)


def project(dst, a, w, transposed=False):
    def body(n):
        cols = at(n * 256, 256)
        dst[:, cols] = dot_nt(a, w[cols, :]) if transposed else dot(a, w[:, cols])

    loop(dst.shape[1] // 256, body)


def normalise(v):
    c = v - jnp.mean(v, axis=-1, keepdims=True)
    rstd = lax.rsqrt(jnp.mean(c * c, axis=-1, keepdims=True) + EPS)
    return c * rstd, rstd


class Comm:
    def __init__(self, g, r, ka=0, kr=0):
        self.g, self.r, self.ka, self.kr = g, r, ka, kr
        self.i = lax.axis_index(DP)
        self.j = lax.axis_index(SEQ)
        self.z, self.y = self.i // g.Y, rem(self.i, g.Y)
        self.x, self.c = self.j // 2, rem(self.j, 2)
        self.pending = []

    def zpeer(self, d):
        return (rem(self.z + d, self.g.Z) * self.g.Y + self.y, self.j)

    def ypeer(self, d):
        return (self.z * self.g.Y + rem(self.y + d, self.g.Y), self.j)

    def xpeer(self, d):
        return (self.i, rem(self.x + d, self.g.X) * 2 + self.c)

    def partner(self):
        return (self.i, self.x * 2 + 1 - self.c)

    def barrier(self):
        g = self.g
        peers = [self.zpeer(d) for d in range(1, g.Z)]
        peers += [self.ypeer(d) for d in range(1, g.Y)]
        peers += [self.xpeer(d) for d in range(1, g.X)]
        peers.append(self.partner())
        sem = pltpu.get_barrier_semaphore()
        for p in peers:
            pl.semaphore_signal(sem, inc=1, device_id=p, device_id_type=MESH)
        pl.semaphore_wait(sem, len(peers))

    def copy(self, src, dst, ss, rs, dev):
        return pltpu.make_async_remote_copy(
            src_ref=src, dst_ref=dst, send_sem=ss, recv_sem=rs, device_id=dev, device_id_type=MESH
        )

    def local(self, src, dst, sem):
        d = pltpu.make_async_copy(src, dst, sem)
        d.start()
        return d

    def when(self, cond, fn):
        if cond is None:
            fn()
        else:
            pl.when(cond)(fn)

    def w_descs(self, p, view, dz):
        r, g = self.r, self.g
        i = rem(self.z - dz + g.Z, g.Z) * g.Y + self.y
        v = view(i)
        return i, [
            self.copy(v, v, r.wys.at[p, d - 1, dz], r.wyr.at[p, d - 1, dz], self.ypeer(d))
            for d in range(1, g.Y)
        ]

    def w_z(self, p, view, d):
        v = view(self.i)
        r = self.r
        return self.copy(v, v, r.wzs.at[p, d - 1], r.wzr.at[p, d - 1], self.zpeer(d))

    def w_start(self, p, view, own=lambda i: None):
        def go():
            for d in range(1, self.g.Z):
                self.w_z(p, view, d).start()

        self.when(own(self.i), go)

    def w_relay(self, p, view, own=lambda i: None):
        r, g = self.r, self.g
        for dz in range(g.Z):
            i, descs = self.w_descs(p, view, dz)

            def go(i=i, descs=descs, dz=dz):
                v = view(i)
                if dz:
                    self.copy(
                        v, v, r.wzs.at[p, dz - 1], r.wzr.at[p, dz - 1], self.zpeer(dz)
                    ).wait_recv()
                for d in descs:
                    d.start()

            self.when(own(i), go)

    def w_finish(self, p, view, own=lambda i: None):
        r, g = self.r, self.g
        for dz in range(g.Z):
            for d in range(1, g.Y):
                i = rem(self.z - dz + g.Z, g.Z) * g.Y + rem(self.y - d + g.Y, g.Y)

                def go(i=i, d=d, dz=dz):
                    v = view(i)
                    self.copy(
                        v, v, r.wys.at[p, d - 1, dz], r.wyr.at[p, d - 1, dz], self.ypeer(d)
                    ).wait_recv()

                self.when(own(i), go)

    def w_drain(self, p, view, own=lambda i: None):
        g = self.g

        def go():
            for d in range(1, g.Z):
                self.w_z(p, view, d).wait_send()

        self.when(own(self.i), go)
        for dz in range(g.Z):
            i, descs = self.w_descs(p, view, dz)

            def go2(descs=descs):
                for d in descs:
                    d.wait_send()

            self.when(own(i), go2)

    def ag_x(self, k, view, d):
        v, r = view(self.j), self.r
        return self.copy(v, v, r.axs.at[self.ka + k, d - 1], r.axr.at[self.ka + k, d - 1], self.xpeer(d))

    def ag_c(self, k, view, d):
        g, r = self.g, self.r
        v = view(rem(self.x - d + g.X, g.X) * 2 + self.c)
        return self.copy(v, v, r.acs.at[self.ka + k, d], r.acr.at[self.ka + k, d], self.partner())

    def ag_start(self, k, view):
        for d in range(1, self.g.X):
            self.ag_x(k, view, d).start()
        self.ag_c(k, view, 0).start()

    def ag_relay(self, k, view):
        g, r = self.g, self.r
        for d in range(1, g.X):
            v = view(rem(self.x - d + g.X, g.X) * 2 + self.c)
            self.copy(
                v, v, r.axs.at[self.ka + k, d - 1], r.axr.at[self.ka + k, d - 1], self.xpeer(d)
            ).wait_recv()
            self.ag_c(k, view, d).start()

    def ag_finish(self, k, view):
        g, r = self.g, self.r
        for d in range(g.X):
            v = view(rem(self.x - d + g.X, g.X) * 2 + 1 - self.c)
            self.copy(v, v, r.acs.at[self.ka + k, d], r.acr.at[self.ka + k, d], self.partner()).wait_recv()

    def ag_drain(self, k, view):
        for d in range(1, self.g.X):
            self.ag_x(k, view, d).wait_send()
        for d in range(self.g.X):
            self.ag_c(k, view, d).wait_send()

    def rs_c(self, k, b, d, cols=None):
        r, k = self.r, k + self.kr
        src, dst = b.ps.at[d], b.pr.at[d]
        if cols is not None:
            src, dst = src.at[:, cols], dst.at[:, cols]
        return self.copy(src, dst, r.rcs.at[k, d], r.rcr.at[k, d], self.partner())

    def rs_x(self, k, b, d, cols=None):
        r, k = self.r, k + self.kr
        src, dst = b.xs.at[d - 1], b.xr.at[d - 1]
        if cols is not None:
            src, dst = src.at[:, cols], dst.at[:, cols]
        return self.copy(src, dst, r.rxs.at[k, d - 1], r.rxr.at[k, d - 1], self.xpeer(d))

    def rs_start(self, k, b, n, part):
        g = self.g
        for d in list(range(1, g.X)) + [0]:
            part(rem(self.x + d, g.X), b.part)
            b.acc[d] = b.part[at(self.c * n, n), :]
            b.ps[d] = b.part[at((1 - self.c) * n, n), :].astype(BF)
            self.rs_c(k, b, d).start()
        self.rs_turn(k, b)

    def rs_start_halves(self, k, b, n, part):
        g = self.g
        for d in list(range(1, g.X)) + [0]:
            first = rem(self.x + d, g.X) * 2 * n
            b.ps[d] = part(at(first + (1 - self.c) * n, n)).astype(BF)
            self.rs_c(k, b, d).start()
            b.acc[d] = part(at(first + self.c * n, n)).astype(b.acc.dtype)

    def rs_turn(self, k, b, cols=None):
        for d in range(1, self.g.X):
            self.rs_c(k, b, d, cols).wait_recv()
            if cols is None:
                b.xs[d - 1] = (b.acc[d][...].astype(F32) + b.pr[d].astype(F32)).astype(BF)
            else:
                total = b.acc[d, :, cols].astype(F32) + b.pr[d, :, cols].astype(F32)
                b.xs[d - 1, :, cols] = total.astype(BF)
            self.rs_x(k, b, d, cols).start()

    def rs_finish(self, k, b, cols=None):
        g = self.g
        here = pl.ds(0, g.D) if cols is None else cols
        self.rs_c(k, b, 0, cols).wait_recv()
        own = b.acc[0][...] if cols is None else b.acc[0, :, cols]
        total = own.astype(F32) + b.pr[0, :, here].astype(F32)
        for d in range(1, g.X):
            self.rs_x(k, b, d, cols).wait_recv()
            total = total + b.xr[d - 1, :, here].astype(F32)
        for d in range(g.X):
            self.rs_c(k, b, d, cols).wait_send()
        for d in range(1, g.X):
            self.rs_x(k, b, d, cols).wait_send()
        return total

    def g_y(self, t, d, dz):
        g, r = self.g, self.r
        p, view, yr, zr, out = t
        i = rem(self.z + dz, g.Z) * g.Y + rem(self.y + d, g.Y)
        return self.copy(
            view(i),
            yr.at[d - 1, dz],
            r.gys.at[p, d - 1, dz],
            r.gyr.at[p, d - 1, dz],
            self.ypeer(d),
        )

    def g_z(self, t, dz):
        g, r = self.g, self.r
        p, view, yr, zr, out = t
        i = rem(self.z + dz, g.Z) * g.Y + self.y
        return self.copy(
            view(i), zr.at[dz - 1], r.gzs.at[p, dz - 1], r.gzr.at[p, dz - 1], self.zpeer(dz)
        )

    def g_start(self, t):
        for dz in list(range(1, self.g.Z)) + [0]:
            for d in range(1, self.g.Y):
                self.g_y(t, d, dz).start()

    def g_sum(self, t, dz):
        g = self.g
        p, view, yr, zr, out = t
        v = view(rem(self.z + dz, g.Z) * g.Y + self.y)
        total = v[...].astype(F32)
        for d in range(1, g.Y):
            self.g_y(t, d, dz).wait_recv()
            total = total + yr[d - 1, dz].astype(F32)
        return v, total

    def g_turn(self, t):
        for dz in range(1, self.g.Z):
            v, total = self.g_sum(t, dz)
            v[...] = total.astype(v.dtype)
            self.g_z(t, dz).start()

    def g_finish(self, t):
        p, view, yr, zr, out = t
        v, total = self.g_sum(t, 0)
        for dz in range(1, self.g.Z):
            self.g_z(t, dz).wait_recv()
            total = total + zr[dz - 1].astype(F32)
        out[...] = total.astype(out.dtype)

    def g_drain(self, t):
        for dz in range(self.g.Z):
            for d in range(1, self.g.Y):
                self.g_y(t, d, dz).wait_send()
        for dz in range(1, self.g.Z):
            self.g_z(t, dz).wait_send()


def attend_forward(g, q_ref, k_ref, v_ref, o_ref, dst, bufs, Lk, causal, limit, between):
    lane = lax.broadcasted_iota(jnp.int32, (1, 128), 1)
    low = lane < HD
    scale = HD ** -0.5
    pbuf, psem = bufs

    def put(t, a, e):
        keys = pl.ds(0, (a + 1) * CH if causal else Lk)
        return pltpu.make_async_copy(
            pbuf.at[2 * t + e, :, keys],
            dst.at[2 * t + e, pl.ds(a * CH, CH), keys],
            psem.at[2 * t + e],
        )

    for a in range(g.L // CH):
        rows = pl.ds(a * CH, CH)
        kk = (a + 1) * CH if causal else Lk
        keys = pl.ds(0, kk)
        col = lax.broadcasted_iota(jnp.int32, (CH, kk), 1)
        if causal:
            ok = col <= lax.broadcasted_iota(jnp.int32, (CH, kk), 0) + a * CH
        else:
            ok = col < limit

        def body(t):
            cols = at(t * 128, 128)
            q = q_ref[rows, cols]
            k = k_ref[keys, cols]
            v = v_ref[keys, cols]
            outs = []
            for e in range(2):
                qe = jnp.where(low if e == 0 else ~low, q, jnp.zeros_like(q))
                s = jnp.where(ok, dot_nt(qe, k) * scale, -1e30)
                ex = jnp.exp(s - jnp.max(s, axis=-1, keepdims=True))
                pb = (ex * (1.0 / jnp.sum(ex, axis=-1, keepdims=True))).astype(BF)
                if a:
                    put(t, a - 1, e).wait()
                pbuf[2 * t + e, :, keys] = pb
                put(t, a, e).start()
                outs.append(dot(pb, v))
            o_ref[rows, cols] = jnp.where(low, outs[0], outs[1]).astype(BF)

        loop(g.NB, body)
        between(a)
    for t in range(g.NB):
        for e in range(2):
            put(t, g.L // CH - 1, e).wait()


def forward_body(g, r, cm, state):
    i, j, x, c = cm.i, cm.j, cm.x, cm.c
    Tl, El, D, Dl, DH, FB = g.Tl, g.El, g.D, g.Dl, g.DH, g.FB
    state.l_og = cm.local(r.out_grad, r.og, r.ls.at[6])

    xv = lambda s: r.x.at[at(s * Tl, Tl), :]
    ev = lambda s: r.enc.at[at(s * El, El), :]
    lx = cm.local(r.tok, xv(j), r.ls.at[0])
    le = cm.local(r.states, ev(j), r.ls.at[1])

    own_rows = at(i * Dl, Dl)

    def col_block(t):
        return pl.ds(pl.multiple_of((t * g.S + j) * 128, 128), 128)

    def stage3(src, dst, sem):
        return [
            cm.local(
                src.at[:, :, col_block(t)], dst.at[:, own_rows, pl.ds(t * 128, 128)], sem.at[t]
            )
            for t in range(g.NB)
        ]

    def so_row(s):
        b = (s * Dl) // 128
        return (b // g.S) * 128 + rem(s * Dl, 128)

    def so_own(s):
        return rem((s * Dl) // 128, g.S) == j

    views = {}
    pieces = []

    def piece(view, own=lambda s: None):
        pieces.append((len(pieces), view, own))
        return pieces[-1]

    if g.wide:
        p_small = piece(lambda s: r.smalls.at[s])
    p_q = [piece(lambda s, n=n: r.wq.at[n, at(s * Dl, Dl), :]) for n in range(3)]
    p_so = piece(lambda s: r.wo.at[at(so_row(s), Dl), :], so_own)
    p_c = [piece(lambda s, n=n: r.wc.at[n, at(s * Dl, Dl), :]) for n in range(3)]
    p_co = piece(lambda s: r.wd.at[at(so_row(s), Dl), :], so_own)
    n1 = g.FJ // 256
    p_1 = [
        piece(lambda s, n=n: r.w1.at[at(s * Dl, Dl), pl.ds(n * 256, 256)]) for n in range(n1)
    ]
    n2 = D // 256
    p_2 = [
        piece(lambda s, n=n: r.w2.at[at(s * FB, FB), pl.ds(n * 256, 256)]) for n in range(n2)
    ]

    st_q = stage3(r.self_qkv, r.wq, r.lq)
    if g.wide:
        f = r.mine
        f[...] = jnp.zeros_like(f)
        nf = g.FF // D
        f[0:6, :] = r.attn_bias[...].astype(F32)
        f[6 : 6 + nf, :] = r.ffn_in_bias[...].astype(F32)
        f[6 + nf : 7 + nf, :] = r.ffn_out_bias[...].astype(F32)
        f[7 + nf : 10 + nf, :] = r.norm_gain[...].astype(F32)
        f[10 + nf : 13 + nf, :] = r.norm_bias[...].astype(F32)
        r.smalls[i] = f[...].astype(BF)

    def stage_row(src, dst, sem, wait):
        def go():
            d = pltpu.make_async_copy(src, dst.at[at(so_row(i), Dl), :], sem)
            if wait:
                d.wait()
            else:
                d.start()

        pl.when(so_own(i))(go)

    stage_row(r.self_out, r.wo, r.ls.at[3], False)
    st_c = stage3(r.cross_qkv, r.wc, r.lc)
    stage_row(r.cross_out, r.wd, r.ls.at[4], False)
    if g.wide:
        st_1 = [
            cm.local(
                r.ffn_in.at[:, pl.ds(pl.multiple_of((t * g.S + j) * 128, 128), 128)],
                r.w1.at[own_rows, pl.ds(t * 128, 128)],
                r.l1.at[t],
            )
            for t in range(g.R)
        ]
    else:
        st_1 = [cm.local(r.ffn_in, r.w1.at[own_rows, :], r.l1.at[0])]
    st_2 = [
        cm.local(r.ffn_out.at[at(j * FB, FB), :], r.w2.at[at(i * FB, FB), :], r.ls.at[5])
    ]

    cm.barrier()
    r.sg[...] = jnp.zeros_like(r.sg)

    lx.wait()
    cm.ag_start(0, xv)
    staged = []
    for n in range(3):
        staged.append((p_q[n], st_q if n == 0 else [], None))
    staged.append((p_so, [], (r.self_out, r.wo, r.ls.at[3])))
    for n in range(3):
        staged.append((p_c[n], st_c if n == 0 else [], None))
    staged.append((p_co, [], (r.cross_out, r.wd, r.ls.at[4])))
    for n in range(n1):
        staged.append((p_1[n], st_1 if n == 0 else [], None))
    for n in range(n2):
        staged.append((p_2[n], st_2 if n == 0 else [], None))

    def start_next():
        if staged:
            p, descs, own_rows_copy = staged.pop(0)
            for d in descs:
                d.wait()
            if own_rows_copy:
                stage_row(*own_rows_copy, True)
            cm.w_start(*p)

    if g.wide:
        cm.w_start(*p_small)
    for _ in range(AHEAD):
        start_next()
    if g.wide:
        cm.w_relay(*p_small)
    cm.ag_relay(0, xv)
    le.wait()
    cm.ag_start(1, ev)
    for p in p_q:
        cm.w_relay(*p)
        start_next()
    cm.ag_relay(1, ev)
    cm.ag_finish(0, xv)
    if g.wide:
        cm.w_finish(*p_small)
        for s in range(g.R):
            r.sm[:, s * 128 : (s + 1) * 128] = r.smalls[s].astype(F32)
        r.fbv[0:1, :] = r.sm[pl.ds(6 + j, 1), :]
    else:
        r.sm[...] = r.small[...].astype(F32)
        r.fbv[0:1, :] = r.fbias[0:1, :]
    nb = 6 + g.FF // D

    def bias_cols(row):
        return jnp.concatenate([r.sm[row : row + 1, col_block(t)] for t in range(g.NB)], axis=1)

    def row_of(n):
        return r.sm[n : n + 1, :]

    queue = [p_so] + p_c + [p_co] + p_1 + p_2

    def relay(count):
        for _ in range(min(count, len(queue))):
            cm.w_relay(*queue.pop(0))
            start_next()

    plan = list(PLAN)

    zero = jnp.zeros((1, DH), F32)
    for n, v in enumerate((bias_cols(0), zero, bias_cols(1), zero, bias_cols(4), bias_cols(3))):
        r.bias[8 * n : 8 * n + 1, :] = v
    relay(plan[0])
    for p in p_q:
        cm.w_finish(*p)

    def qkv(n):
        r.qkv[n] = (dot(r.x[...], r.wq[n]) + r.bias[pl.ds(n * 8, 1), :]).astype(BF)

    loop(3, qkv)
    relay(plan[1])
    save_x = cm.local(r.x, r.o_x, r.ls.at[7])

    def between_self(a):
        relay(plan[2 + min(a, 1)])

    attend_forward(
        g,
        r.qkv.at[0],
        r.qkv.at[1],
        r.qkv.at[2],
        r.sof.at[j],
        r.o_pbs,
        (r.pbuf, r.psem),
        g.L,
        True,
        None,
        between_self,
    )
    cm.w_finish(*p_so)

    buf = types.SimpleNamespace(part=r.part, acc=r.acc, ps=r.ps, pr=r.pr, xs=r.xs, xr=r.xr)

    def projected(src, w):
        def part(xx, dst):
            project(dst, src[at(xx * 2 * Tl, 2 * Tl), :], w)

        return part

    cm.rs_start(0, buf, Tl, projected(r.sof.at[j], r.wo))
    relay(plan[4])
    branch = cm.rs_finish(0, buf) + row_of(2)
    hat, rstd = normalise(xv(j)[...].astype(F32) + branch)
    r.h1[...] = hat
    r.rs1[...] = jnp.broadcast_to(rstd, (Tl, 128))
    first = hat * row_of(nb + 1) + row_of(nb + 4)
    r.dh[...] = first
    fv = lambda s: r.fb.at[at(s * Tl, Tl), :]
    r.fb[at(j * Tl, Tl), :] = first.astype(BF)
    cm.ag_start(2, fv)

    cm.ag_finish(1, ev)
    relay(plan[5])
    for p in p_c:
        cm.w_finish(*p)

    def ckv(n):
        y = dot(r.enc[...], r.wc[n + 1]) + r.bias[pl.ds(n * 8 + 24, 1), :]
        r.ckv[n] = y.astype(BF)

    loop(2, ckv)
    cm.ag_relay(2, fv)
    cm.ag_finish(2, fv)
    r.cq[...] = (dot(r.fb[...], r.wc[0]) + r.bias[40:41, :]).astype(BF)

    sov = lambda s: r.sof.at[s]
    cov = lambda s: r.cof.at[s]
    cm.ag_start(4, sov)

    relay(plan[6])

    def between_cross(a):
        if a == 0:
            cm.ag_relay(4, sov)
        relay(plan[7 + min(a, 1)])

    attend_forward(
        g,
        r.cq,
        r.ckv.at[0],
        r.ckv.at[1],
        r.cof.at[j],
        r.o_pbc,
        (r.pbuf, r.psem),
        g.E,
        False,
        r.lens[1],
        between_cross,
    )
    cm.w_finish(*p_co)
    save_x.wait()
    cm.ag_drain(0, xv)
    cm.rs_start(1, buf, Tl, projected(r.cof.at[j], r.wd))
    relay(plan[9])
    branch = cm.rs_finish(1, buf) + row_of(5)
    hat, rstd = normalise(r.dh[...] + branch)
    r.h2[...] = hat
    r.rs2[...] = jnp.broadcast_to(rstd, (Tl, 128))
    second = hat * row_of(nb + 2) + row_of(nb + 5)
    r.dh[...] = second
    sv = lambda s: r.x.at[at(s * Tl, Tl), :]
    r.x[at(j * Tl, Tl), :] = second.astype(BF)
    cm.ag_start(3, sv)

    relay(plan[10])
    cm.ag_relay(3, sv)
    relay(plan[11])
    cm.ag_finish(3, sv)
    cm.ag_start(5, cov)
    cm.ag_finish(4, sov)
    while len(queue) > n2 or staged:
        relay(1)
    first1 = p_1[0][0]

    def piece1(n):
        return first1 + n, lambda s: r.w1.at[at(s * Dl, Dl), at(n * 256, 256)]

    def hidden(n):
        cm.w_finish(*piece1(n))
        cols = at(n * 256, 256)
        pre = dot(r.x[...], r.w1[:, cols]) + r.fbv[0:1, cols]
        cdf = 0.5 * (1.0 + lax.erf(pre * 0.7071067811865476))
        r.hid[:, cols] = (pre * cdf).astype(BF)
        r.dg[:, cols] = (cdf + pre * jnp.exp(-0.5 * pre * pre) * 0.3989422804014327).astype(BF)

    half = n1 // 2
    loop(half, hidden)
    relay(plan[12])
    loop(n1 - half, lambda n: hidden(n + half))
    cm.ag_relay(5, cov)
    relay(len(queue))
    for p in p_2:
        cm.w_finish(*p)
    cm.rs_start(2, buf, Tl, projected(r.hid, r.w2))
    cm.ag_finish(5, cov)
    branch = cm.rs_finish(2, buf) + row_of(nb)
    hat, rstd = normalise(r.dh[...] + branch)
    r.h3[...] = hat
    r.rs3[...] = jnp.broadcast_to(rstd, (Tl, 128))
    third = hat * row_of(nb + 3) + row_of(nb + 6)
    row = j * Tl + lax.broadcasted_iota(jnp.int32, (Tl, 1), 0)
    live = (row < r.lens[0]).astype(F32)
    r.lo[...] = (third * live).astype(BF)
    state.outs.append(cm.local(r.lo, r.o_lo, r.ls.at[8]))

    def drain():
        for p in pieces:
            cm.w_drain(*p)
        for k, v in ((2, fv), (4, sov), (5, cov)):
            cm.ag_drain(k, v)

    state.drain = drain
    state.drain_second = lambda: cm.ag_drain(3, sv)
    state.drain_states = lambda: cm.ag_drain(1, ev)
    state.live = live


def attend_backward(g, q_ref, k_ref, v_ref, do_ref, src, bufs, outs, acc, Lk, causal, between):
    lane = lax.broadcasted_iota(jnp.int32, (1, 128), 1)
    low = lane < HD
    scale = HD ** -0.5
    dq_ref, dk_ref, dv_ref = outs
    dka, dva = acc
    pbuf, psem = bufs
    top = g.L // CH - 1

    def width(a):
        return (a + 1) * CH if causal else Lk

    def fetch(t, a, e):
        kk = width(a)
        return pltpu.make_async_copy(
            src.at[2 * t + e, pl.ds(a * CH, CH), pl.ds(0, kk)],
            pbuf.at[2 * t + e, :, pl.ds(0, kk)],
            psem.at[2 * t + e],
        )

    for t in range(g.NB):
        for e in range(2):
            fetch(t, top, e).start()
    for a in range(top, -1, -1):
        rows = pl.ds(a * CH, CH)
        kk = width(a)
        keys = pl.ds(0, kk)

        def body(t):
            cols = at(t * 128, 128)
            q = q_ref[rows, cols]
            do = do_ref[rows, cols]
            k = k_ref[keys, cols]
            v = v_ref[keys, cols]
            zero = jnp.zeros_like(q)
            dqs = []
            for e in range(2):
                fetch(t, a, e).wait()
                mine = low if e == 0 else ~low
                qe = jnp.where(mine, q, zero)
                doe = jnp.where(mine, do, zero)
                p = pbuf[2 * t + e, :, keys]
                pf = p.astype(F32)
                w = dot_nt(doe, v) * pf
                ds = (w - pf * jnp.sum(w, axis=-1, keepdims=True)).astype(BF)
                dqs.append(dot(ds, k))
                dk = dot_tn(ds, qe)
                dv = dot_tn(p, doe)
                if a:
                    fetch(t, a - 1, e).start()
                if a == top and e == 0:
                    dka[t, keys, :] = dk
                    dva[t, keys, :] = dv
                else:
                    dka[t, keys, :] += dk
                    dva[t, keys, :] += dv
            dq_ref[rows, cols] = (jnp.where(low, dqs[0], dqs[1]) * scale).astype(BF)

        loop(g.NB, body)
        between(a)

    def finish(t):
        cols = at(t * 128, 128)
        keys = pl.ds(0, Lk)
        dk_ref[keys, cols] = (dka[t, keys, :] * scale).astype(BF)
        dv_ref[keys, cols] = dva[t, keys, :].astype(BF)

    loop(g.NB, finish)


class Rows:
    def __init__(self, ref, first, size):
        self.ref, self.first, self.size, self.dtype = ref, first, size, ref.dtype
        self.at = self

    def rows(self, d):
        return pl.ds((self.first + d) * self.size, self.size)

    def __getitem__(self, d):
        return self.ref.at[self.rows(d), :]

    def __setitem__(self, d, value):
        self.ref[self.rows(d), :] = value


def colsum(v):
    return jnp.sum(v.astype(F32), axis=0, keepdims=True)


def backward_body(g, r, cm, state):
    i, j, c = cm.i, cm.j, cm.c
    Tl, El, D, Dl, DH, FB, FJ = g.Tl, g.El, g.D, g.Dl, g.DH, g.FB, g.FJ
    nb = 6 + g.FF // D

    def col_block(t):
        return pl.ds(pl.multiple_of((t * g.S + j) * 128, 128), 128)

    def put_cols(row, value):
        for t in range(g.NB):
            r.sg[row : row + 1, col_block(t)] = value[:, t * 128 : (t + 1) * 128]

    own = at(j * Tl, Tl)

    def norm_back(gr, hat, rstd, n):
        r.sg[nb + 1 + n : nb + 2 + n, :] = jnp.sum(gr * hat, axis=0, keepdims=True)
        r.sg[nb + 4 + n : nb + 5 + n, :] = jnp.sum(gr, axis=0, keepdims=True)
        gn = gr * r.sm[nb + 1 + n : nb + 2 + n, :]
        return rstd[:, 0:1] * (
            gn
            - jnp.mean(gn, axis=-1, keepdims=True)
            - hat * jnp.mean(gn * hat, axis=-1, keepdims=True)
        )

    def send_dy(k, dh, buf, bias_row):
        low = dh.astype(BF)
        buf[own, :] = low
        view = lambda s: buf.at[at(s * Tl, Tl), :]
        cm.ag_start(k, view)
        r.sg[bias_row : bias_row + 1, :] = colsum(low)
        return view

    n1 = FJ // 256
    n2 = D // 256
    tasks = []

    def task(view, yr, zr, out):
        tasks.append((len(tasks), view, yr, zr, out))
        return tasks[-1]

    t_2 = [
        task(
            lambda s, n=n: r.d2.at[at(s * FB, FB), pl.ds(n * 256, 256)],
            r.yr2.at[n],
            r.zr2.at[n],
            r.g2.at[j, :, pl.ds(n * 256, 256)],
        )
        for n in range(n2)
    ]
    t_1 = [
        task(
            lambda s, n=n: r.d1.at[at(s * Dl, Dl), pl.ds(n * 256, 256)],
            r.yr1.at[n],
            r.zr1.at[n],
            r.g1.at[j, :, pl.ds(n * 256, 256)],
        )
        for n in range(n1)
    ]
    t_c = [
        task(
            lambda s, n=n: r.dc.at[n, at(s * Dl, Dl), :], r.yrc.at[n], r.zrc.at[n], r.gc.at[j, n]
        )
        for n in range(4)
    ]
    t_s = [
        task(
            lambda s, n=n: r.ds.at[n, at(s * Dl, Dl), :], r.yrs.at[n], r.zrs.at[n], r.gs.at[j, n]
        )
        for n in range(4)
    ]
    if g.wide:
        t_g = task(
            lambda s: r.sg.at[:, pl.ds(pl.multiple_of(s * 128, 128), 128)],
            r.yrg,
            r.zrg,
            r.gg.at[j],
        )
    waiting, turns, ends = [], [], []

    def pump():
        while waiting and len(turns) < AHEAD_Y:
            t = waiting.pop(0)
            cm.g_start(t)
            turns.append(t)

    def launch(*ts):
        waiting.extend(ts)
        pump()

    def turn(count):
        for _ in range(min(count, len(turns) + len(waiting))):
            t = turns.pop(0)
            cm.g_turn(t)
            ends.append(t)
            pump()

    def complete(group):
        for t in group:
            while t not in ends:
                turn(1)
            cm.g_finish(t)
            ends.remove(t)

    points = list(BPLAN)

    def point():
        turn(points.pop(0) if points else 0)

    outs = state.outs
    outs2 = []
    finals = []

    def save(src, dst):
        outs.append(cm.local(src, dst, r.os.at[len(outs)]))

    def save_2(s):
        return [(r.g2.at[s], r.o_f2.at[at(s * FB, FB), :])]

    def save_1(s):
        if not g.wide:
            return [(r.g1.at[s], r.o_f1.at[s])]
        return [
            (r.g1.at[s, :, pl.ds(t * 128, 128)], r.o_f1.at[:, at((t * g.S + s) * 128, 128)])
            for t in range(g.R)
        ]

    def save_n(src, d3, d1, parts=range(4)):
        def pairs(s):
            res = []
            for t in range(g.NB):
                cols = at((t * g.S + s) * 128, 128)
                mine = pl.ds(t * 128, 128)
                for n in parts:
                    dst = d3.at[n, :, cols] if n < 3 else d1.at[:, cols]
                    res.append((src.at[s, n, :, mine], dst))
            return res

        return pairs

    def gather(k, view, pairs):
        cm.ag_start(k, view)
        finals.append((k, view, pairs))

    def flush():
        for k, view, pairs in finals:
            cm.ag_finish(k, view)
            todo = [pair for s in range(g.S) for pair in pairs(s)]
            for n, (src, dst) in enumerate(todo):
                outs2.append(cm.local(src, dst, r.fs.at[k - 3, n]))

    state.l_og.wait()
    g3 = r.og[...].astype(F32) * state.live
    dh3 = norm_back(g3, r.h3[...], r.rs3[...], 2)
    r.dh[...] = dh3
    v3 = send_dy(0, dh3, r.dya, nb)

    cm.ag_relay(0, v3)
    cm.ag_finish(0, v3)

    def grad_2(n):
        cols = at(n * 256, 256)
        r.d2[:, cols] = dot_tn(r.hid[...], r.dya[:, cols]).astype(BF)

    def hidden_back(n):
        cols = at(n * 256, 256)
        y = dot_nt(r.dya[...], r.w2[cols, :]) * r.dg[:, cols].astype(F32)
        y = y.astype(BF)
        r.dpre[:, cols] = y
        r.fsum[0:1, cols] = colsum(y)

    grad_2(0)
    launch(t_2[0])
    loop(n2 - 1, lambda n: grad_2(n + 1))
    launch(*t_2[1:])
    loop(n1, hidden_back)
    point()
    if g.wide:
        r.sg[pl.ds(6 + j, 1), :] = r.fsum[0:1, :]
    else:
        r.fg[...] = r.fsum[...]

    def part3(xx, dst):
        project(dst, r.dpre[at(xx * 2 * Tl, 2 * Tl), :], r.w1, True)

    buf = types.SimpleNamespace(part=r.part, acc=r.acc, ps=r.ps, pr=r.pr, xs=r.xs, xr=r.xr)
    cm.rs_start(0, buf, Tl, part3)
    point()

    def grad_1(n):
        cols = at(n * 256, 256)
        r.d1[:, cols] = dot_tn(r.x[...], r.dpre[:, cols]).astype(BF)

    loop(n1, grad_1)
    state.drain_second()
    l_x = cm.local(r.o_x, r.x, r.ls.at[9])
    launch(*t_1)
    point()
    dh2 = norm_back(r.dh[...] + cm.rs_finish(0, buf), r.h2[...], r.rs2[...], 1)
    r.dh[...] = dh2
    v2 = send_dy(1, dh2, r.dyb, 5)
    point()
    cm.ag_relay(1, v2)
    point()

    cm.ag_finish(1, v2)
    r.do[...] = dot_nt(r.dyb[...], r.wd[...]).astype(BF)
    point()

    def between_cross(a):
        point()

    attend_backward(
        g,
        r.cq,
        r.ckv.at[0],
        r.ckv.at[1],
        r.do,
        r.o_pbc,
        (r.pbuf, r.psem),
        (r.dcq, r.dckv.at[0], r.dckv.at[1]),
        (r.dka, r.dva),
        g.E,
        False,
        between_cross,
    )

    def part4(xx, dst):
        project(dst, r.dcq[at(xx * 2 * Tl, 2 * Tl), :], r.wc.at[0], True)

    cm.ag_drain(0, v3)
    cm.rs_start(1, buf, Tl, part4)
    point()
    put_cols(3, colsum(r.dcq[...]))
    put_cols(4, colsum(r.dckv[1]))

    def grad_rows(dst, a, b):
        def body(n):
            rows = at(n * 256, 256)
            dst[rows, :] = dot_tn(a[:, rows], b[...]).astype(BF)

        loop(D // 256, body)

    def grad_out(full, dy, dst):
        dyj = jnp.concatenate([dy[:, col_block(t)] for t in range(g.NB)], axis=1)

        def body(s):
            y = dot_tn(full[s], dyj).astype(BF)
            for t in range(g.NB):
                dst[at((t * g.S + s) * 128, 128), :] = y[t * 128 : (t + 1) * 128, :]

        loop(g.S, body)

    grad_out(r.cof, r.dyb, r.dc.at[3])
    launch(t_c[3])
    grad_rows(r.dc.at[1], r.enc, r.dckv.at[0])
    launch(t_c[1])
    point()
    dh1 = norm_back(r.dh[...] + cm.rs_finish(1, buf), r.h1[...], r.rs1[...], 0)
    r.dh[...] = dh1
    v1 = send_dy(2, dh1, r.dya, 2)
    point()
    grad_rows(r.dc.at[2], r.enc, r.dckv.at[1])
    launch(t_c[2])
    point()
    cm.ag_relay(2, v1)
    grad_rows(r.dc.at[0], r.fb, r.dcq)
    launch(t_c[0])
    point()
    complete(t_2)
    gather(3, lambda s: r.g2.at[s], save_2)
    ebuf = types.SimpleNamespace(
        acc=Rows(r.enc, 0, El), ps=Rows(r.enc, g.X, El), pr=r.epr, xs=r.exs, xr=r.exr
    )

    def part_e(rows):
        return dot_nt(r.dckv[0, rows, :], r.wc[1]) + dot_nt(r.dckv[1, rows, :], r.wc[2])

    point()

    cm.ag_finish(2, v1)
    r.do[...] = dot_nt(r.dya[...], r.wo[...]).astype(BF)
    grad_out(r.sof, r.dya, r.ds.at[3])
    launch(t_s[3])
    point()
    state.drain_states()
    cm.rs_start_halves(3, ebuf, El, part_e)
    complete(t_1)
    gather(4, lambda s: r.g1.at[s], save_1)

    def between_self(a):
        if a == g.L // CH - 1:
            cm.ag_relay(*finals[0][:2])
            cm.rs_turn(3, ebuf)
        point()

    attend_backward(
        g,
        r.qkv.at[0],
        r.qkv.at[1],
        r.qkv.at[2],
        r.do,
        r.o_pbs,
        (r.pbuf, r.psem),
        (r.dqkv.at[0], r.dqkv.at[1], r.dqkv.at[2]),
        (r.dka, r.dva),
        g.L,
        True,
        between_self,
    )

    def part5(xx, dst):
        rows = at(xx * 2 * Tl, 2 * Tl)

        def body(n):
            cols = at(n * 256, 256)
            dst[:, cols] = (
                dot_nt(r.dqkv[0, rows, :], r.wq[0, cols, :])
                + dot_nt(r.dqkv[1, rows, :], r.wq[1, cols, :])
                + dot_nt(r.dqkv[2, rows, :], r.wq[2, cols, :])
            )

        loop(D // 256, body)

    l_x.wait()
    put_cols(0, colsum(r.dqkv[0]))
    put_cols(1, colsum(r.dqkv[2]))
    if g.wide:
        launch(t_g)
    for n in range(3):
        grad_rows(r.ds.at[n], r.x, r.dqkv.at[n])
        launch(t_s[n])
        point()
    cm.rs_start(2, buf, Tl, part5)
    cm.ag_relay(*finals[1][:2])
    complete([t_c[n] for n in (3, 1, 2, 0)])
    gather(5, lambda s: r.gc.at[s], save_n(r.gc, r.o_cq, r.o_co))
    r.ge[...] = cm.rs_finish(3, ebuf).astype(BF)
    save(r.ge, r.o_ge)
    r.gi[...] = (r.dh[...] + cm.rs_finish(2, buf)).astype(BF)
    save(r.gi, r.o_gi)
    order = [3, 0, 1, 2]
    for m, n in enumerate(order):
        complete([t_s[n]])
        gather(6 + n, lambda s, n=n: r.gs.at[s, n], save_n(r.gs, r.o_sq, r.o_so, [n]))
        cm.ag_relay(*finals[m + 2][:2])
        if n == 3 and g.wide:
            complete([t_g])
            cm.ag_start(10, lambda s: r.gg.at[s])
    cm.ag_relay(*finals[6][:2])
    v_gg = lambda s: r.gg.at[s]
    if g.wide:
        cm.ag_relay(10, v_gg)
        cm.ag_finish(10, v_gg)
    flush()
    if g.wide:
        total = r.gg[0]
        for s in range(1, g.S):
            total = total + r.gg[s]
        r.gsum[...] = total
        save(r.gsum, r.o_small)
    else:
        save(r.sg, r.o_small)
        save(r.fg, r.o_fg)

    cm.ag_drain(1, v2)
    cm.ag_drain(2, v1)
    for k, view, pairs in finals:
        cm.ag_drain(k, view)
    if g.wide:
        cm.ag_drain(10, v_gg)
    for t in tasks:
        cm.g_drain(t)
    state.drain()
    for d in outs + outs2:
        d.wait()


def whole_kernel(g, names, *refs):
    r = types.SimpleNamespace(**dict(zip(names, refs)))
    state = types.SimpleNamespace(outs=[])
    forward_body(g, r, Comm(g, r), state)
    backward_body(g, r, Comm(g, r, 6, 2 + g.D // 256), state)


def whole_call(g, ins):
    names, in_specs, args = [], [], []
    for n, a in ins.items():
        names.append(n)
        args.append(a)
        if n == LENS:
            in_specs.append(pl.BlockSpec(memory_space=pltpu.SMEM))
        elif a.size <= 8 * FJ_MAX:
            in_specs.append(pl.BlockSpec(memory_space=pltpu.VMEM))
        else:
            in_specs.append(ANY)
    D, L, E, Tl, El, S = g.D, g.L, g.E, g.Tl, g.El, g.S
    Dl, DH, FJ, FB = g.Dl, g.DH, g.FJ, g.FB
    V = pltpu.VMEM
    outs = dict(
        lo=((Tl, D), BF),
        x=((L, D), BF),
        pbs=((g.H, L, L), BF),
        pbc=((g.H, L, E), BF),
        gi=((Tl, D), BF),
        ge=((El, D), BF),
        f2=((g.FR, D), BF),
        f1=((Dl, g.FF) if g.wide else (S, Dl, FJ), BF),
        cq=((3, Dl, D), BF),
        co=((Dl, D), BF),
        sq=((3, Dl, D), BF),
        so=((Dl, D), BF),
        small=((NS, 128) if g.wide else (NS, D), F32),
    )
    if not g.wide:
        outs.update(fg=((8, FJ), F32))
    names += ["o_" + n for n in outs]
    scratch = dict(
        lo=V((Tl, D), BF),
        x=V((L, D), BF),
        enc=V((E, D), BF),
        wq=V((3, D, DH), BF),
        wo=V((DH, D), BF),
        wc=V((3, D, DH), BF),
        wd=V((DH, D), BF),
        w1=V((D, FJ), BF),
        w2=V((FJ, D), BF),
        sm=V((NS, D), F32),
        qkv=V((3, L, DH), BF),
        sof=V((S, L, DH), BF),
        fb=V((L, D), BF),
        cq=V((L, DH), BF),
        ckv=V((2, E, DH), BF),
        cof=V((S, L, DH), BF),
        hid=V((L, FJ), BF),
        dg=V((L, FJ), BF),
        h1=V((Tl, D), F32),
        h2=V((Tl, D), F32),
        h3=V((Tl, D), F32),
        rs1=V((Tl, 128), F32),
        rs2=V((Tl, 128), F32),
        rs3=V((Tl, 128), F32),
        bias=V((48, DH), F32),
        fbv=V((8, FJ), F32),
        gi=V((Tl, D), BF),
        ge=V((El, D), BF),
        g2=V((S, FB, D), BF),
        g1=V((S, Dl, FJ), BF),
        gc=V((S, 4, Dl, DH), BF),
        gs=V((S, 4, Dl, DH), BF),
        fsum=V((8, FJ), F32),
    )
    two = V((g.X, Tl, D), BF)
    one = V((g.X - 1, Tl, D), BF)
    scratch.update(
        og=V((Tl, D), BF),
        dh=V((Tl, D), F32),
        sg=V((NS, D), F32),
        part=V((2 * Tl, D), F32),
        acc=V((g.X, Tl, D), F32),
        ps=two,
        pr=two,
        xs=one,
        xr=one,
        epr=V((g.X, El, D), BF),
        exs=V((g.X - 1, El, D), BF),
        exr=V((g.X - 1, El, D), BF),
        dya=V((L, D), BF),
        dyb=V((L, D), BF),
        dpre=V((L, FJ), BF),
        do=V((L, DH), BF),
        dcq=V((L, DH), BF),
        dckv=V((2, E, DH), BF),
        dqkv=V((3, L, DH), BF),
        dka=V((g.NB, E, 128), F32),
        dva=V((g.NB, E, 128), F32),
        pbuf=V((2 * g.NB, CH, E), BF),
        d2=V((FJ, D), BF),
        d1=V((D, FJ), BF),
        dc=V((4, D, DH), BF),
        ds=V((4, D, DH), BF),
        yr2=V((D // 256, g.Y - 1, g.Z, FB, 256), BF),
        yr1=V((FJ // 256, g.Y - 1, g.Z, Dl, 256), BF),
        yrc=V((4, g.Y - 1, g.Z, Dl, DH), BF),
        yrs=V((4, g.Y - 1, g.Z, Dl, DH), BF),
        zr2=V((D // 256, g.Z - 1, FB, 256), BF),
        zr1=V((FJ // 256, g.Z - 1, Dl, 256), BF),
        zrc=V((4, g.Z - 1, Dl, DH), BF),
        zrs=V((4, g.Z - 1, Dl, DH), BF),
    )
    if not g.wide:
        scratch.update(fg=V((8, FJ), F32))
    if g.wide:
        scratch.update(
            smalls=V((g.R, NS, 128), BF),
            mine=V((NS, 128), F32),
            yrg=V((g.Y - 1, g.Z, NS, 128), F32),
            zrg=V((g.Z - 1, NS, 128), F32),
            gg=V((S, NS, 128), F32),
            gsum=V((NS, 128), F32),
        )
    sem = pltpu.SemaphoreType.DMA
    NP = 9 + FJ // 256 + D // 256
    scratch.update(
        ls=sem((10,)),
        lq=sem((g.NB,)),
        lc=sem((g.NB,)),
        l1=sem((g.R,)),
        wzs=sem((NP, g.Z - 1)),
        wzr=sem((NP, g.Z - 1)),
        wys=sem((NP, g.Y - 1, g.Z)),
        wyr=sem((NP, g.Y - 1, g.Z)),
        os=sem((8,)),
        psem=sem((2 * g.NB,)),
        fs=sem((7, max(S * (g.R if g.wide else 1), 4 * S * g.NB))),
        gys=sem((NP, g.Y - 1, g.Z)),
        gyr=sem((NP, g.Y - 1, g.Z)),
        gzs=sem((NP, g.Z - 1)),
        gzr=sem((NP, g.Z - 1)),
        axs=sem((17, g.X - 1)),
        axr=sem((17, g.X - 1)),
        acs=sem((17, g.X)),
        acr=sem((17, g.X)),
        rcs=sem((6 + D // 256, g.X)),
        rcr=sem((6 + D // 256, g.X)),
        rxs=sem((6 + D // 256, g.X - 1)),
        rxr=sem((6 + D // 256, g.X - 1)),
    )
    names += list(scratch)
    out = pl.pallas_call(
        functools.partial(whole_kernel, g, names),
        out_shape=[jax.ShapeDtypeStruct(*s) for s in outs.values()],
        in_specs=in_specs,
        out_specs=[ANY] * len(outs),
        scratch_shapes=list(scratch.values()),
        compiler_params=pltpu.CompilerParams(
            collective_id=0, has_side_effects=True, vmem_limit_bytes=67043328
        ),
    )(*args)
    return dict(zip(outs, out))


def finish_kernel(cuts, *refs):
    half = (len(refs) - len(cuts)) // 2
    ins, small = refs[:half], refs[half]
    outs, smalls = refs[half + 1 : 2 * half + 1], refs[2 * half + 1 :]
    for src, dst in zip(ins, outs):
        dst[...] = src[...].astype(dst.dtype)
    for (lo, hi), dst in zip(cuts, smalls):
        dst[...] = small[lo:hi, :]


def finish_call(g, parts, small):
    steps = 4 if g.Dl % 64 == 0 else 2
    nf = g.FF // g.D
    cuts = ((0, 6), (6, 6 + nf), (6 + nf, 7 + nf), (7 + nf, 10 + nf), (10 + nf, 13 + nf))
    specs, shapes = [], []
    for n, (a, dtype) in enumerate(parts):
        block = list(a.shape)
        block[-2] //= steps
        lead = a.ndim - 2
        specs.append(pl.BlockSpec(tuple(block), lambda k, lead=lead: (0,) * lead + (k, 0)))
        shapes.append(jax.ShapeDtypeStruct(a.shape, dtype))
    for lo, hi in cuts:
        shapes.append(jax.ShapeDtypeStruct((hi - lo, small.shape[1]), F32))

    def whole(shape):
        return pl.BlockSpec(shape, lambda k: (0, 0))

    return pl.pallas_call(
        functools.partial(finish_kernel, cuts),
        grid=(steps,),
        out_shape=shapes,
        in_specs=specs + [whole(small.shape)],
        out_specs=specs + [whole(s.shape) for s in shapes[len(specs) :]],
        compiler_params=pltpu.CompilerParams(vmem_limit_bytes=67043328),
    )(*[a for a, _ in parts], small)


def on_device(
    decoder_in,
    encoder_states,
    out_grad,
    seq_lengths,
    enc_lengths,
    self_qkv,
    self_out,
    cross_qkv,
    cross_out,
    attn_bias,
    ffn_in,
    ffn_in_bias,
    ffn_out,
    ffn_out_bias,
    norm_gain,
    norm_bias,
):
    R = lax.axis_size(DP)
    S = lax.axis_size(SEQ)
    j = lax.axis_index(SEQ)
    D = decoder_in.shape[2]
    FF = ffn_in.shape[1]
    g = configure(R, S, decoder_in.shape[1], encoder_states.shape[1], D, FF)
    Dl, FR, FB, FJ, NB = g.Dl, g.FR, g.FB, g.FJ, g.NB
    nf = FF // D
    nb = 6 + nf

    fi, fo = ffn_in_bias.reshape(nf, Dl), ffn_out_bias.reshape(1, Dl)
    lens = jnp.concatenate([seq_lengths, enc_lengths])
    ins = dict(
        lens=lens,
        tok=decoder_in[0],
        states=encoder_states[0],
        out_grad=out_grad[0],
        self_qkv=self_qkv,
        self_out=self_out,
        cross_qkv=cross_qkv,
        cross_out=cross_out,
        ffn_in=ffn_in,
        ffn_out=ffn_out,
    )
    if g.wide:
        ins.update(
            attn_bias=attn_bias,
            ffn_in_bias=fi,
            ffn_out_bias=fo,
            norm_gain=norm_gain,
            norm_bias=norm_bias,
        )
    else:
        pad = jnp.zeros((NS - nb - 7, Dl), BF)
        small = jnp.concatenate([attn_bias, fi, fo, norm_gain, norm_bias, pad])
        small = lax.all_gather(small, DP, axis=1, tiled=True)
        fb = small[6:nb].reshape(nf, R, Dl).transpose(1, 0, 2)
        fb = lax.dynamic_slice_in_dim(fb.reshape(R, FR), j * FB, FB, axis=1).reshape(1, -1)
        packed = lax.dynamic_slice_in_dim(ffn_in.reshape(Dl, R, FR), j * FB, FB, axis=2)
        ins.update(
            small=small,
            fbias=jnp.broadcast_to(fb.astype(F32), (8, FJ)),
            ffn_in=packed.reshape(Dl, FJ),
        )
    b = types.SimpleNamespace(**whole_call(g, ins))

    sm = b.small
    if not g.wide:
        fpl = lax.dynamic_update_slice(
            jnp.zeros((R, S, FB), F32), b.fg[0].reshape(R, 1, FB), (0, j, 0)
        )
        fpl = fpl.reshape(R, nf, Dl).transpose(1, 0, 2).reshape(nf, D)
        sm = lax.dynamic_update_slice(sm, fpl, (6, 0))
        sm = lax.psum(lax.psum_scatter(sm, DP, scatter_dimension=1, tiled=True), SEQ)

    gw1 = b.f1
    if not g.wide:
        gw1 = gw1.reshape(S, Dl, R, FB).transpose(1, 2, 0, 3).reshape(Dl, FF)
    parts = [(b.lo, BF), (b.gi, BF), (b.ge, BF)]
    parts += [(a, F32) for a in (b.sq, b.so, b.cq, b.co, gw1, b.f2)]
    lo, gi, ge, sq, so, cq, co, f1, f2, gab, gfi, gfo, ggain, gshift = finish_call(g, parts, sm)
    return (
        lo[None],
        gi[None],
        ge[None],
        sq,
        so,
        cq,
        co,
        gab,
        f1,
        gfi.reshape(-1),
        f2,
        gfo.reshape(-1),
        ggain,
        gshift,
    )


def solution(mesh):
    act = P(DP, SEQ, None)
    w3 = P(None, DP, None)
    w2 = P(DP, None)
    v2 = P(None, DP)
    v1 = P(DP)
    return jax.shard_map(
        on_device,
        mesh=mesh,
        in_specs=(act, act, act, v1, v1, w3, w2, w3, w2, v2, w2, v1, w2, v1, v2, v2),
        out_specs=(act, act, act, w3, w2, w3, w2, v2, w2, v1, w2, v1, v2, v2),
        check_vma=False,
    )
```

```python
import functools
import types

import jax
import jax.numpy as jnp
from jax import lax
from jax.experimental import pallas as pl
from jax.experimental.pallas import tpu as pltpu
from jax.sharding import PartitionSpec as P

HD = 64
EPS = 1e-05
F32 = jnp.float32
BF = jnp.bfloat16
MESH = pl.DeviceIdType.MESH
ANY = pl.BlockSpec(memory_space=pl.ANY)
CH = 256
NS = 32
DP = "dp"
SEQ = "seq"
LENS = "lens"
FJ_MAX = 4096
AHEAD = 2
AHEAD_Y = 2
PLAN = (1, 1, 1, 1, 2, 1, 1, 1, 1, 1, 1, 0, 1)
BPLAN = (0, 1, 1, 1, 0, 1, 1, 1, 1, 0, 1, 0, 1, 0, 1, 1, 1, 0, 1, 1)


def configure(R, S, Tl, El, D, FF):
    g = types.SimpleNamespace(R=R, S=S, Tl=Tl, El=El, D=D, FF=FF)
    g.Y = 1
    while 8 * g.Y * g.Y <= R:
        g.Y *= 2
    g.Z = R // g.Y
    g.X = S // 2
    g.Dl = D // R
    g.FR = FF // R
    g.FB = g.FR // S
    g.DH = D // S
    g.FJ = FF // S
    g.NB = g.DH // 128
    g.H = g.DH // HD
    g.L = Tl * S
    g.E = El * S
    g.wide = g.Dl == 128 and g.FB == 128
    return g


def dot(a, b):
    return jnp.dot(a, b, preferred_element_type=F32)


def dot_nt(a, b):
    return lax.dot_general(a, b, (((1,), (1,)), ((), ())), preferred_element_type=F32)


def dot_tn(a, b):
    return lax.dot_general(a, b, (((0,), (0,)), ((), ())), preferred_element_type=F32)


def rem(a, b):
    return lax.rem(a, jnp.int32(b))


def at(start, size):
    if isinstance(start, int):
        return pl.ds(start, size)
    return pl.ds(pl.multiple_of(start, size), size)


def loop(count, body):
    if count == 1:
        body(0)
    else:
        lax.fori_loop(0, count, lambda n, z: (body(n), z)[1], 0)


def project(dst, a, w, transposed=False):
    def body(n):
        cols = at(n * 256, 256)
        dst[:, cols] = dot_nt(a, w[cols, :]) if transposed else dot(a, w[:, cols])

    loop(dst.shape[1] // 256, body)


def normalise(v):
    c = v - jnp.mean(v, axis=-1, keepdims=True)
    rstd = lax.rsqrt(jnp.mean(c * c, axis=-1, keepdims=True) + EPS)
    return c * rstd, rstd


class Comm:
    def __init__(self, g, r, ka=0, kr=0):
        self.g, self.r, self.ka, self.kr = g, r, ka, kr
        self.i = lax.axis_index(DP)
        self.j = lax.axis_index(SEQ)
        self.z, self.y = self.i // g.Y, rem(self.i, g.Y)
        self.x, self.c = self.j // 2, rem(self.j, 2)
        self.pending = []

    def zpeer(self, d):
        return (rem(self.z + d, self.g.Z) * self.g.Y + self.y, self.j)

    def ypeer(self, d):
        return (self.z * self.g.Y + rem(self.y + d, self.g.Y), self.j)

    def xpeer(self, d):
        return (self.i, rem(self.x + d, self.g.X) * 2 + self.c)

    def partner(self):
        return (self.i, self.x * 2 + 1 - self.c)

    def barrier(self):
        g = self.g
        peers = [self.zpeer(d) for d in range(1, g.Z)]
        peers += [self.ypeer(d) for d in range(1, g.Y)]
        peers += [self.xpeer(d) for d in range(1, g.X)]
        peers.append(self.partner())
        sem = pltpu.get_barrier_semaphore()
        for p in peers:
            pl.semaphore_signal(sem, inc=1, device_id=p, device_id_type=MESH)
        pl.semaphore_wait(sem, len(peers))

    def copy(self, src, dst, ss, rs, dev):
        return pltpu.make_async_remote_copy(
            src_ref=src, dst_ref=dst, send_sem=ss, recv_sem=rs, device_id=dev, device_id_type=MESH
        )

    def local(self, src, dst, sem):
        d = pltpu.make_async_copy(src, dst, sem)
        d.start()
        return d

    def when(self, cond, fn):
        if cond is None:
            fn()
        else:
            pl.when(cond)(fn)

    def w_descs(self, p, view, dz):
        r, g = self.r, self.g
        i = rem(self.z - dz + g.Z, g.Z) * g.Y + self.y
        v = view(i)
        return i, [
            self.copy(v, v, r.wys.at[p, d - 1, dz], r.wyr.at[p, d - 1, dz], self.ypeer(d))
            for d in range(1, g.Y)
        ]

    def w_z(self, p, view, d):
        v = view(self.i)
        r = self.r
        return self.copy(v, v, r.wzs.at[p, d - 1], r.wzr.at[p, d - 1], self.zpeer(d))

    def w_start(self, p, view, own=lambda i: None):
        def go():
            for d in range(1, self.g.Z):
                self.w_z(p, view, d).start()

        self.when(own(self.i), go)

    def w_relay(self, p, view, own=lambda i: None):
        r, g = self.r, self.g
        for dz in range(g.Z):
            i, descs = self.w_descs(p, view, dz)

            def go(i=i, descs=descs, dz=dz):
                v = view(i)
                if dz:
                    self.copy(
                        v, v, r.wzs.at[p, dz - 1], r.wzr.at[p, dz - 1], self.zpeer(dz)
                    ).wait_recv()
                for d in descs:
                    d.start()

            self.when(own(i), go)

    def w_finish(self, p, view, own=lambda i: None):
        r, g = self.r, self.g
        for dz in range(g.Z):
            for d in range(1, g.Y):
                i = rem(self.z - dz + g.Z, g.Z) * g.Y + rem(self.y - d + g.Y, g.Y)

                def go(i=i, d=d, dz=dz):
                    v = view(i)
                    self.copy(
                        v, v, r.wys.at[p, d - 1, dz], r.wyr.at[p, d - 1, dz], self.ypeer(d)
                    ).wait_recv()

                self.when(own(i), go)

    def w_drain(self, p, view, own=lambda i: None):
        g = self.g

        def go():
            for d in range(1, g.Z):
                self.w_z(p, view, d).wait_send()

        self.when(own(self.i), go)
        for dz in range(g.Z):
            i, descs = self.w_descs(p, view, dz)

            def go2(descs=descs):
                for d in descs:
                    d.wait_send()

            self.when(own(i), go2)

    def ag_x(self, k, view, d):
        v, r = view(self.j), self.r
        return self.copy(v, v, r.axs.at[self.ka + k, d - 1], r.axr.at[self.ka + k, d - 1], self.xpeer(d))

    def ag_c(self, k, view, d):
        g, r = self.g, self.r
        v = view(rem(self.x - d + g.X, g.X) * 2 + self.c)
        return self.copy(v, v, r.acs.at[self.ka + k, d], r.acr.at[self.ka + k, d], self.partner())

    def ag_start(self, k, view):
        for d in range(1, self.g.X):
            self.ag_x(k, view, d).start()
        self.ag_c(k, view, 0).start()

    def ag_relay(self, k, view):
        g, r = self.g, self.r
        for d in range(1, g.X):
            v = view(rem(self.x - d + g.X, g.X) * 2 + self.c)
            self.copy(
                v, v, r.axs.at[self.ka + k, d - 1], r.axr.at[self.ka + k, d - 1], self.xpeer(d)
            ).wait_recv()
            self.ag_c(k, view, d).start()

    def ag_finish(self, k, view):
        g, r = self.g, self.r
        for d in range(g.X):
            v = view(rem(self.x - d + g.X, g.X) * 2 + 1 - self.c)
            self.copy(v, v, r.acs.at[self.ka + k, d], r.acr.at[self.ka + k, d], self.partner()).wait_recv()

    def ag_drain(self, k, view):
        for d in range(1, self.g.X):
            self.ag_x(k, view, d).wait_send()
        for d in range(self.g.X):
            self.ag_c(k, view, d).wait_send()

    def rs_c(self, k, b, d, cols=None):
        r, k = self.r, k + self.kr
        src, dst = b.ps.at[d], b.pr.at[d]
        if cols is not None:
            src, dst = src.at[:, cols], dst.at[:, cols]
        return self.copy(src, dst, r.rcs.at[k, d], r.rcr.at[k, d], self.partner())

    def rs_x(self, k, b, d, cols=None):
        r, k = self.r, k + self.kr
        src, dst = b.xs.at[d - 1], b.xr.at[d - 1]
        if cols is not None:
            src, dst = src.at[:, cols], dst.at[:, cols]
        return self.copy(src, dst, r.rxs.at[k, d - 1], r.rxr.at[k, d - 1], self.xpeer(d))

    def rs_start(self, k, b, n, part):
        g = self.g
        for d in list(range(1, g.X)) + [0]:
            part(rem(self.x + d, g.X), b.part)
            b.acc[d] = b.part[at(self.c * n, n), :]
            b.ps[d] = b.part[at((1 - self.c) * n, n), :].astype(BF)
            self.rs_c(k, b, d).start()
        self.rs_turn(k, b)

    def rs_start_halves(self, k, b, n, part):
        g = self.g
        for d in list(range(1, g.X)) + [0]:
            first = rem(self.x + d, g.X) * 2 * n
            b.ps[d] = part(at(first + (1 - self.c) * n, n)).astype(BF)
            self.rs_c(k, b, d).start()
            b.acc[d] = part(at(first + self.c * n, n)).astype(b.acc.dtype)

    def rs_turn(self, k, b, cols=None):
        for d in range(1, self.g.X):
            self.rs_c(k, b, d, cols).wait_recv()
            if cols is None:
                b.xs[d - 1] = (b.acc[d][...].astype(F32) + b.pr[d].astype(F32)).astype(BF)
            else:
                total = b.acc[d, :, cols].astype(F32) + b.pr[d, :, cols].astype(F32)
                b.xs[d - 1, :, cols] = total.astype(BF)
            self.rs_x(k, b, d, cols).start()

    def rs_finish(self, k, b, cols=None):
        g = self.g
        here = pl.ds(0, g.D) if cols is None else cols
        self.rs_c(k, b, 0, cols).wait_recv()
        own = b.acc[0][...] if cols is None else b.acc[0, :, cols]
        total = own.astype(F32) + b.pr[0, :, here].astype(F32)
        for d in range(1, g.X):
            self.rs_x(k, b, d, cols).wait_recv()
            total = total + b.xr[d - 1, :, here].astype(F32)
        for d in range(g.X):
            self.rs_c(k, b, d, cols).wait_send()
        for d in range(1, g.X):
            self.rs_x(k, b, d, cols).wait_send()
        return total

    def g_y(self, t, d, dz):
        g, r = self.g, self.r
        p, view, yr, zr, out = t
        i = rem(self.z + dz, g.Z) * g.Y + rem(self.y + d, g.Y)
        return self.copy(
            view(i),
            yr.at[d - 1, dz],
            r.gys.at[p, d - 1, dz],
            r.gyr.at[p, d - 1, dz],
            self.ypeer(d),
        )

    def g_z(self, t, dz):
        g, r = self.g, self.r
        p, view, yr, zr, out = t
        i = rem(self.z + dz, g.Z) * g.Y + self.y
        return self.copy(
            view(i), zr.at[dz - 1], r.gzs.at[p, dz - 1], r.gzr.at[p, dz - 1], self.zpeer(dz)
        )

    def g_start(self, t):
        for dz in list(range(1, self.g.Z)) + [0]:
            for d in range(1, self.g.Y):
                self.g_y(t, d, dz).start()

    def g_sum(self, t, dz):
        g = self.g
        p, view, yr, zr, out = t
        v = view(rem(self.z + dz, g.Z) * g.Y + self.y)
        total = v[...].astype(F32)
        for d in range(1, g.Y):
            self.g_y(t, d, dz).wait_recv()
            total = total + yr[d - 1, dz].astype(F32)
        return v, total

    def g_turn(self, t):
        for dz in range(1, self.g.Z):
            v, total = self.g_sum(t, dz)
            v[...] = total.astype(v.dtype)
            self.g_z(t, dz).start()

    def g_finish(self, t):
        p, view, yr, zr, out = t
        v, total = self.g_sum(t, 0)
        for dz in range(1, self.g.Z):
            self.g_z(t, dz).wait_recv()
            total = total + zr[dz - 1].astype(F32)
        out[...] = total.astype(out.dtype)

    def g_drain(self, t):
        for dz in range(self.g.Z):
            for d in range(1, self.g.Y):
                self.g_y(t, d, dz).wait_send()
        for dz in range(1, self.g.Z):
            self.g_z(t, dz).wait_send()


def attend_forward(g, q_ref, k_ref, v_ref, o_ref, dst, bufs, Lk, causal, limit, between):
    lane = lax.broadcasted_iota(jnp.int32, (1, 128), 1)
    low = lane < HD
    scale = HD ** -0.5
    pbuf, psem = bufs

    def put(t, a, e):
        keys = pl.ds(0, (a + 1) * CH if causal else Lk)
        return pltpu.make_async_copy(
            pbuf.at[2 * t + e, :, keys],
            dst.at[2 * t + e, pl.ds(a * CH, CH), keys],
            psem.at[2 * t + e],
        )

    for a in range(g.L // CH):
        rows = pl.ds(a * CH, CH)
        kk = (a + 1) * CH if causal else Lk
        keys = pl.ds(0, kk)
        col = lax.broadcasted_iota(jnp.int32, (CH, kk), 1)
        if causal:
            ok = col <= lax.broadcasted_iota(jnp.int32, (CH, kk), 0) + a * CH
        else:
            ok = col < limit

        def body(t):
            cols = at(t * 128, 128)
            q = q_ref[rows, cols]
            k = k_ref[keys, cols]
            v = v_ref[keys, cols]
            outs = []
            for e in range(2):
                qe = jnp.where(low if e == 0 else ~low, q, jnp.zeros_like(q))
                s = jnp.where(ok, dot_nt(qe, k) * scale, -1e30)
                ex = jnp.exp(s - jnp.max(s, axis=-1, keepdims=True))
                pb = (ex * (1.0 / jnp.sum(ex, axis=-1, keepdims=True))).astype(BF)
                if a:
                    put(t, a - 1, e).wait()
                pbuf[2 * t + e, :, keys] = pb
                put(t, a, e).start()
                outs.append(dot(pb, v))
            o_ref[rows, cols] = jnp.where(low, outs[0], outs[1]).astype(BF)

        loop(g.NB, body)
        between(a)
    for t in range(g.NB):
        for e in range(2):
            put(t, g.L // CH - 1, e).wait()


def forward_body(g, r, cm, state):
    i, j, x, c = cm.i, cm.j, cm.x, cm.c
    Tl, El, D, Dl, DH, FB = g.Tl, g.El, g.D, g.Dl, g.DH, g.FB
    state.l_og = cm.local(r.out_grad, r.og, r.ls.at[6])

    xv = lambda s: r.x.at[at(s * Tl, Tl), :]
    ev = lambda s: r.enc.at[at(s * El, El), :]
    lx = cm.local(r.tok, xv(j), r.ls.at[0])
    le = cm.local(r.states, ev(j), r.ls.at[1])

    own_rows = at(i * Dl, Dl)

    def col_block(t):
        return pl.ds(pl.multiple_of((t * g.S + j) * 128, 128), 128)

    def stage3(src, dst, sem):
        return [
            cm.local(
                src.at[:, :, col_block(t)], dst.at[:, own_rows, pl.ds(t * 128, 128)], sem.at[t]
            )
            for t in range(g.NB)
        ]

    def so_row(s):
        b = (s * Dl) // 128
        return (b // g.S) * 128 + rem(s * Dl, 128)

    def so_own(s):
        return rem((s * Dl) // 128, g.S) == j

    views = {}
    pieces = []

    def piece(view, own=lambda s: None):
        pieces.append((len(pieces), view, own))
        return pieces[-1]

    if g.wide:
        p_small = piece(lambda s: r.smalls.at[s])
    p_q = [piece(lambda s, n=n: r.wq.at[n, at(s * Dl, Dl), :]) for n in range(3)]
    p_so = piece(lambda s: r.wo.at[at(so_row(s), Dl), :], so_own)
    p_c = [piece(lambda s, n=n: r.wc.at[n, at(s * Dl, Dl), :]) for n in range(3)]
    p_co = piece(lambda s: r.wd.at[at(so_row(s), Dl), :], so_own)
    n1 = g.FJ // 256
    p_1 = [
        piece(lambda s, n=n: r.w1.at[at(s * Dl, Dl), pl.ds(n * 256, 256)]) for n in range(n1)
    ]
    n2 = D // 256
    p_2 = [
        piece(lambda s, n=n: r.w2.at[at(s * FB, FB), pl.ds(n * 256, 256)]) for n in range(n2)
    ]

    st_q = stage3(r.self_qkv, r.wq, r.lq)
    if g.wide:
        f = r.mine
        f[...] = jnp.zeros_like(f)
        nf = g.FF // D
        f[0:6, :] = r.attn_bias[...].astype(F32)
        f[6 : 6 + nf, :] = r.ffn_in_bias[...].astype(F32)
        f[6 + nf : 7 + nf, :] = r.ffn_out_bias[...].astype(F32)
        f[7 + nf : 10 + nf, :] = r.norm_gain[...].astype(F32)
        f[10 + nf : 13 + nf, :] = r.norm_bias[...].astype(F32)
        r.smalls[i] = f[...].astype(BF)

    def stage_row(src, dst, sem, wait):
        def go():
            d = pltpu.make_async_copy(src, dst.at[at(so_row(i), Dl), :], sem)
            if wait:
                d.wait()
            else:
                d.start()

        pl.when(so_own(i))(go)

    stage_row(r.self_out, r.wo, r.ls.at[3], False)
    st_c = stage3(r.cross_qkv, r.wc, r.lc)
    stage_row(r.cross_out, r.wd, r.ls.at[4], False)
    if g.wide:
        st_1 = [
            cm.local(
                r.ffn_in.at[:, pl.ds(pl.multiple_of((t * g.S + j) * 128, 128), 128)],
                r.w1.at[own_rows, pl.ds(t * 128, 128)],
                r.l1.at[t],
            )
            for t in range(g.R)
        ]
    else:
        st_1 = [cm.local(r.ffn_in, r.w1.at[own_rows, :], r.l1.at[0])]
    st_2 = [
        cm.local(r.ffn_out.at[at(j * FB, FB), :], r.w2.at[at(i * FB, FB), :], r.ls.at[5])
    ]

    cm.barrier()
    r.sg[...] = jnp.zeros_like(r.sg)

    lx.wait()
    cm.ag_start(0, xv)
    staged = []
    for n in range(3):
        staged.append((p_q[n], st_q if n == 0 else [], None))
    staged.append((p_so, [], (r.self_out, r.wo, r.ls.at[3])))
    for n in range(3):
        staged.append((p_c[n], st_c if n == 0 else [], None))
    staged.append((p_co, [], (r.cross_out, r.wd, r.ls.at[4])))
    for n in range(n1):
        staged.append((p_1[n], st_1 if n == 0 else [], None))
    for n in range(n2):
        staged.append((p_2[n], st_2 if n == 0 else [], None))

    def start_next():
        if staged:
            p, descs, own_rows_copy = staged.pop(0)
            for d in descs:
                d.wait()
            if own_rows_copy:
                stage_row(*own_rows_copy, True)
            cm.w_start(*p)

    if g.wide:
        cm.w_start(*p_small)
    for _ in range(AHEAD):
        start_next()
    if g.wide:
        cm.w_relay(*p_small)
    cm.ag_relay(0, xv)
    le.wait()
    cm.ag_start(1, ev)
    for p in p_q:
        cm.w_relay(*p)
        start_next()
    cm.ag_relay(1, ev)
    cm.ag_finish(0, xv)
    if g.wide:
        cm.w_finish(*p_small)
        for s in range(g.R):
            r.sm[:, s * 128 : (s + 1) * 128] = r.smalls[s].astype(F32)
        r.fbv[0:1, :] = r.sm[pl.ds(6 + j, 1), :]
    else:
        r.sm[...] = r.small[...].astype(F32)
        r.fbv[0:1, :] = r.fbias[0:1, :]
    nb = 6 + g.FF // D

    def bias_cols(row):
        return jnp.concatenate([r.sm[row : row + 1, col_block(t)] for t in range(g.NB)], axis=1)

    def row_of(n):
        return r.sm[n : n + 1, :]

    queue = [p_so] + p_c + [p_co] + p_1 + p_2

    def relay(count):
        for _ in range(min(count, len(queue))):
            cm.w_relay(*queue.pop(0))
            start_next()

    plan = list(PLAN)

    zero = jnp.zeros((1, DH), F32)
    for n, v in enumerate((bias_cols(0), zero, bias_cols(1), zero, bias_cols(4), bias_cols(3))):
        r.bias[8 * n : 8 * n + 1, :] = v
    relay(plan[0])
    for p in p_q:
        cm.w_finish(*p)

    def qkv(n):
        r.qkv[n] = (dot(r.x[...], r.wq[n]) + r.bias[pl.ds(n * 8, 1), :]).astype(BF)

    loop(3, qkv)
    relay(plan[1])
    save_x = cm.local(r.x, r.o_x, r.ls.at[7])

    def between_self(a):
        relay(plan[2 + min(a, 1)])

    attend_forward(
        g,
        r.qkv.at[0],
        r.qkv.at[1],
        r.qkv.at[2],
        r.sof.at[j],
        r.o_pbs,
        (r.pbuf, r.psem),
        g.L,
        True,
        None,
        between_self,
    )
    cm.w_finish(*p_so)

    buf = types.SimpleNamespace(part=r.part, acc=r.acc, ps=r.ps, pr=r.pr, xs=r.xs, xr=r.xr)

    def projected(src, w):
        def part(xx, dst):
            project(dst, src[at(xx * 2 * Tl, 2 * Tl), :], w)

        return part

    cm.rs_start(0, buf, Tl, projected(r.sof.at[j], r.wo))
    relay(plan[4])
    branch = cm.rs_finish(0, buf) + row_of(2)
    hat, rstd = normalise(xv(j)[...].astype(F32) + branch)
    r.h1[...] = hat
    r.rs1[...] = jnp.broadcast_to(rstd, (Tl, 128))
    first = hat * row_of(nb + 1) + row_of(nb + 4)
    r.dh[...] = first
    fv = lambda s: r.fb.at[at(s * Tl, Tl), :]
    r.fb[at(j * Tl, Tl), :] = first.astype(BF)
    cm.ag_start(2, fv)

    cm.ag_finish(1, ev)
    relay(plan[5])
    for p in p_c:
        cm.w_finish(*p)

    def ckv(n):
        y = dot(r.enc[...], r.wc[n + 1]) + r.bias[pl.ds(n * 8 + 24, 1), :]
        r.ckv[n] = y.astype(BF)

    loop(2, ckv)
    cm.ag_relay(2, fv)
    cm.ag_finish(2, fv)
    r.cq[...] = (dot(r.fb[...], r.wc[0]) + r.bias[40:41, :]).astype(BF)

    sov = lambda s: r.sof.at[s]
    cov = lambda s: r.cof.at[s]
    cm.ag_start(4, sov)

    relay(plan[6])

    def between_cross(a):
        if a == 0:
            cm.ag_relay(4, sov)
        relay(plan[7 + min(a, 1)])

    attend_forward(
        g,
        r.cq,
        r.ckv.at[0],
        r.ckv.at[1],
        r.cof.at[j],
        r.o_pbc,
        (r.pbuf, r.psem),
        g.E,
        False,
        r.lens[1],
        between_cross,
    )
    cm.w_finish(*p_co)
    save_x.wait()
    cm.ag_drain(0, xv)
    cm.rs_start(1, buf, Tl, projected(r.cof.at[j], r.wd))
    relay(plan[9])
    branch = cm.rs_finish(1, buf) + row_of(5)
    hat, rstd = normalise(r.dh[...] + branch)
    r.h2[...] = hat
    r.rs2[...] = jnp.broadcast_to(rstd, (Tl, 128))
    second = hat * row_of(nb + 2) + row_of(nb + 5)
    r.dh[...] = second
    sv = lambda s: r.x.at[at(s * Tl, Tl), :]
    r.x[at(j * Tl, Tl), :] = second.astype(BF)
    cm.ag_start(3, sv)

    relay(plan[10])
    cm.ag_relay(3, sv)
    relay(plan[11])
    cm.ag_finish(3, sv)
    cm.ag_start(5, cov)
    cm.ag_finish(4, sov)
    while len(queue) > n2 or staged:
        relay(1)
    first1 = p_1[0][0]

    def piece1(n):
        return first1 + n, lambda s: r.w1.at[at(s * Dl, Dl), at(n * 256, 256)]

    def hidden(n):
        cm.w_finish(*piece1(n))
        cols = at(n * 256, 256)
        pre = dot(r.x[...], r.w1[:, cols]) + r.fbv[0:1, cols]
        cdf = 0.5 * (1.0 + lax.erf(pre * 0.7071067811865476))
        r.hid[:, cols] = (pre * cdf).astype(BF)
        r.dg[:, cols] = (cdf + pre * jnp.exp(-0.5 * pre * pre) * 0.3989422804014327).astype(BF)

    half = n1 // 2
    loop(half, hidden)
    relay(plan[12])
    loop(n1 - half, lambda n: hidden(n + half))
    cm.ag_relay(5, cov)
    relay(len(queue))
    for p in p_2:
        cm.w_finish(*p)
    cm.rs_start(2, buf, Tl, projected(r.hid, r.w2))
    cm.ag_finish(5, cov)
    branch = cm.rs_finish(2, buf) + row_of(nb)
    hat, rstd = normalise(r.dh[...] + branch)
    r.h3[...] = hat
    r.rs3[...] = jnp.broadcast_to(rstd, (Tl, 128))
    third = hat * row_of(nb + 3) + row_of(nb + 6)
    row = j * Tl + lax.broadcasted_iota(jnp.int32, (Tl, 1), 0)
    live = (row < r.lens[0]).astype(F32)
    r.lo[...] = (third * live).astype(BF)
    state.outs.append(cm.local(r.lo, r.o_lo, r.ls.at[8]))

    def drain():
        for p in pieces:
            cm.w_drain(*p)
        for k, v in ((2, fv), (4, sov), (5, cov)):
            cm.ag_drain(k, v)

    state.drain = drain
    state.drain_second = lambda: cm.ag_drain(3, sv)
    state.drain_states = lambda: cm.ag_drain(1, ev)
    state.live = live


def attend_backward(g, q_ref, k_ref, v_ref, do_ref, src, bufs, outs, acc, Lk, causal, between):
    lane = lax.broadcasted_iota(jnp.int32, (1, 128), 1)
    low = lane < HD
    scale = HD ** -0.5
    dq_ref, dk_ref, dv_ref = outs
    dka, dva = acc
    pbuf, psem = bufs
    top = g.L // CH - 1

    def width(a):
        return (a + 1) * CH if causal else Lk

    def fetch(t, a, e):
        kk = width(a)
        return pltpu.make_async_copy(
            src.at[2 * t + e, pl.ds(a * CH, CH), pl.ds(0, kk)],
            pbuf.at[2 * t + e, :, pl.ds(0, kk)],
            psem.at[2 * t + e],
        )

    for t in range(g.NB):
        for e in range(2):
            fetch(t, top, e).start()
    for a in range(top, -1, -1):
        rows = pl.ds(a * CH, CH)
        kk = width(a)
        keys = pl.ds(0, kk)

        def body(t):
            cols = at(t * 128, 128)
            q = q_ref[rows, cols]
            do = do_ref[rows, cols]
            k = k_ref[keys, cols]
            v = v_ref[keys, cols]
            zero = jnp.zeros_like(q)
            dqs = []
            for e in range(2):
                fetch(t, a, e).wait()
                mine = low if e == 0 else ~low
                qe = jnp.where(mine, q, zero)
                doe = jnp.where(mine, do, zero)
                p = pbuf[2 * t + e, :, keys]
                pf = p.astype(F32)
                w = dot_nt(doe, v) * pf
                ds = (w - pf * jnp.sum(w, axis=-1, keepdims=True)).astype(BF)
                dqs.append(dot(ds, k))
                dk = dot_tn(ds, qe)
                dv = dot_tn(p, doe)
                if a:
                    fetch(t, a - 1, e).start()
                if a == top and e == 0:
                    dka[t, keys, :] = dk
                    dva[t, keys, :] = dv
                else:
                    dka[t, keys, :] += dk
                    dva[t, keys, :] += dv
            dq_ref[rows, cols] = (jnp.where(low, dqs[0], dqs[1]) * scale).astype(BF)

        loop(g.NB, body)
        between(a)

    def finish(t):
        cols = at(t * 128, 128)
        keys = pl.ds(0, Lk)
        dk_ref[keys, cols] = (dka[t, keys, :] * scale).astype(BF)
        dv_ref[keys, cols] = dva[t, keys, :].astype(BF)

    loop(g.NB, finish)


class Rows:
    def __init__(self, ref, first, size):
        self.ref, self.first, self.size, self.dtype = ref, first, size, ref.dtype
        self.at = self

    def rows(self, d):
        return pl.ds((self.first + d) * self.size, self.size)

    def __getitem__(self, d):
        return self.ref.at[self.rows(d), :]

    def __setitem__(self, d, value):
        self.ref[self.rows(d), :] = value


def colsum(v):
    return jnp.sum(v.astype(F32), axis=0, keepdims=True)


def backward_body(g, r, cm, state):
    i, j, c = cm.i, cm.j, cm.c
    Tl, El, D, Dl, DH, FB, FJ = g.Tl, g.El, g.D, g.Dl, g.DH, g.FB, g.FJ
    nb = 6 + g.FF // D

    def col_block(t):
        return pl.ds(pl.multiple_of((t * g.S + j) * 128, 128), 128)

    def put_cols(row, value):
        for t in range(g.NB):
            r.sg[row : row + 1, col_block(t)] = value[:, t * 128 : (t + 1) * 128]

    own = at(j * Tl, Tl)

    def norm_back(gr, hat, rstd, n):
        r.sg[nb + 1 + n : nb + 2 + n, :] = jnp.sum(gr * hat, axis=0, keepdims=True)
        r.sg[nb + 4 + n : nb + 5 + n, :] = jnp.sum(gr, axis=0, keepdims=True)
        gn = gr * r.sm[nb + 1 + n : nb + 2 + n, :]
        return rstd[:, 0:1] * (
            gn
            - jnp.mean(gn, axis=-1, keepdims=True)
            - hat * jnp.mean(gn * hat, axis=-1, keepdims=True)
        )

    def send_dy(k, dh, buf, bias_row):
        low = dh.astype(BF)
        buf[own, :] = low
        view = lambda s: buf.at[at(s * Tl, Tl), :]
        cm.ag_start(k, view)
        r.sg[bias_row : bias_row + 1, :] = colsum(low)
        return view

    n1 = FJ // 256
    n2 = D // 256
    tasks = []

    def task(view, yr, zr, out):
        tasks.append((len(tasks), view, yr, zr, out))
        return tasks[-1]

    t_2 = [
        task(
            lambda s, n=n: r.d2.at[at(s * FB, FB), pl.ds(n * 256, 256)],
            r.yr2.at[n],
            r.zr2.at[n],
            r.g2.at[j, :, pl.ds(n * 256, 256)],
        )
        for n in range(n2)
    ]
    t_1 = [
        task(
            lambda s, n=n: r.d1.at[at(s * Dl, Dl), pl.ds(n * 256, 256)],
            r.yr1.at[n],
            r.zr1.at[n],
            r.g1.at[j, :, pl.ds(n * 256, 256)],
        )
        for n in range(n1)
    ]
    t_c = [
        task(
            lambda s, n=n: r.dc.at[n, at(s * Dl, Dl), :], r.yrc.at[n], r.zrc.at[n], r.gc.at[j, n]
        )
        for n in range(4)
    ]
    t_s = [
        task(
            lambda s, n=n: r.ds.at[n, at(s * Dl, Dl), :], r.yrs.at[n], r.zrs.at[n], r.gs.at[j, n]
        )
        for n in range(4)
    ]
    if g.wide:
        t_g = task(
            lambda s: r.sg.at[:, pl.ds(pl.multiple_of(s * 128, 128), 128)],
            r.yrg,
            r.zrg,
            r.gg.at[j],
        )
    waiting, turns, ends = [], [], []

    def pump():
        while waiting and len(turns) < AHEAD_Y:
            t = waiting.pop(0)
            cm.g_start(t)
            turns.append(t)

    def launch(*ts):
        waiting.extend(ts)
        pump()

    def turn(count):
        for _ in range(min(count, len(turns) + len(waiting))):
            t = turns.pop(0)
            cm.g_turn(t)
            ends.append(t)
            pump()

    def complete(group):
        for t in group:
            while t not in ends:
                turn(1)
            cm.g_finish(t)
            ends.remove(t)

    points = list(BPLAN)

    def point():
        turn(points.pop(0) if points else 0)

    outs = state.outs
    outs2 = []
    finals = []

    def save(src, dst):
        outs.append(cm.local(src, dst, r.os.at[len(outs)]))

    def save_2(s):
        return [(r.g2.at[s], r.o_f2.at[at(s * FB, FB), :])]

    def save_1(s):
        if not g.wide:
            return [(r.g1.at[s], r.o_f1.at[s])]
        return [
            (r.g1.at[s, :, pl.ds(t * 128, 128)], r.o_f1.at[:, at((t * g.S + s) * 128, 128)])
            for t in range(g.R)
        ]

    def save_n(src, d3, d1, parts=range(4)):
        def pairs(s):
            res = []
            for t in range(g.NB):
                cols = at((t * g.S + s) * 128, 128)
                mine = pl.ds(t * 128, 128)
                for n in parts:
                    dst = d3.at[n, :, cols] if n < 3 else d1.at[:, cols]
                    res.append((src.at[s, n, :, mine], dst))
            return res

        return pairs

    def gather(k, view, pairs):
        cm.ag_start(k, view)
        finals.append((k, view, pairs))

    def flush():
        for k, view, pairs in finals:
            cm.ag_finish(k, view)
            todo = [pair for s in range(g.S) for pair in pairs(s)]
            for n, (src, dst) in enumerate(todo):
                outs2.append(cm.local(src, dst, r.fs.at[k - 3, n]))

    state.l_og.wait()
    g3 = r.og[...].astype(F32) * state.live
    dh3 = norm_back(g3, r.h3[...], r.rs3[...], 2)
    r.dh[...] = dh3
    v3 = send_dy(0, dh3, r.dya, nb)

    cm.ag_relay(0, v3)
    cm.ag_finish(0, v3)

    def grad_2(n):
        cols = at(n * 256, 256)
        r.d2[:, cols] = dot_tn(r.hid[...], r.dya[:, cols]).astype(BF)

    def hidden_back(n):
        cols = at(n * 256, 256)
        y = dot_nt(r.dya[...], r.w2[cols, :]) * r.dg[:, cols].astype(F32)
        y = y.astype(BF)
        r.dpre[:, cols] = y
        r.fsum[0:1, cols] = colsum(y)

    loop(2, grad_2)
    launch(*t_2[:2])
    loop(n1, hidden_back)
    point()
    if g.wide:
        r.sg[pl.ds(6 + j, 1), :] = r.fsum[0:1, :]
    else:
        r.fg[...] = r.fsum[...]

    def part3(xx, dst):
        project(dst, r.dpre[at(xx * 2 * Tl, 2 * Tl), :], r.w1, True)

    buf = types.SimpleNamespace(part=r.part, acc=r.acc, ps=r.ps, pr=r.pr, xs=r.xs, xr=r.xr)
    cm.rs_start(0, buf, Tl, part3)
    loop(n2 - 2, lambda n: grad_2(n + 2))
    launch(*t_2[2:])
    point()

    def grad_1(n):
        cols = at(n * 256, 256)
        r.d1[:, cols] = dot_tn(r.x[...], r.dpre[:, cols]).astype(BF)

    loop(n1, grad_1)
    state.drain_second()
    l_x = cm.local(r.o_x, r.x, r.ls.at[9])
    launch(*t_1)
    point()
    dh2 = norm_back(r.dh[...] + cm.rs_finish(0, buf), r.h2[...], r.rs2[...], 1)
    r.dh[...] = dh2
    v2 = send_dy(1, dh2, r.dyb, 5)
    point()
    cm.ag_relay(1, v2)
    point()

    cm.ag_finish(1, v2)
    r.do[...] = dot_nt(r.dyb[...], r.wd[...]).astype(BF)
    point()

    def between_cross(a):
        point()

    attend_backward(
        g,
        r.cq,
        r.ckv.at[0],
        r.ckv.at[1],
        r.do,
        r.o_pbc,
        (r.pbuf, r.psem),
        (r.dcq, r.dckv.at[0], r.dckv.at[1]),
        (r.dka, r.dva),
        g.E,
        False,
        between_cross,
    )

    def part4(xx, dst):
        project(dst, r.dcq[at(xx * 2 * Tl, 2 * Tl), :], r.wc.at[0], True)

    cm.ag_drain(0, v3)
    cm.rs_start(1, buf, Tl, part4)
    point()
    put_cols(3, colsum(r.dcq[...]))
    put_cols(4, colsum(r.dckv[1]))

    def grad_rows(dst, a, b):
        def body(n):
            rows = at(n * 256, 256)
            dst[rows, :] = dot_tn(a[:, rows], b[...]).astype(BF)

        loop(D // 256, body)

    def grad_out(full, dy, dst):
        dyj = jnp.concatenate([dy[:, col_block(t)] for t in range(g.NB)], axis=1)

        def body(s):
            y = dot_tn(full[s], dyj).astype(BF)
            for t in range(g.NB):
                dst[at((t * g.S + s) * 128, 128), :] = y[t * 128 : (t + 1) * 128, :]

        loop(g.S, body)

    grad_out(r.cof, r.dyb, r.dc.at[3])
    launch(t_c[3])
    grad_rows(r.dc.at[1], r.enc, r.dckv.at[0])
    launch(t_c[1])
    point()
    dh1 = norm_back(r.dh[...] + cm.rs_finish(1, buf), r.h1[...], r.rs1[...], 0)
    r.dh[...] = dh1
    v1 = send_dy(2, dh1, r.dya, 2)
    point()
    grad_rows(r.dc.at[2], r.enc, r.dckv.at[1])
    launch(t_c[2])
    point()
    cm.ag_relay(2, v1)
    grad_rows(r.dc.at[0], r.fb, r.dcq)
    launch(t_c[0])
    point()
    complete(t_2)
    gather(3, lambda s: r.g2.at[s], save_2)
    ebuf = types.SimpleNamespace(
        acc=Rows(r.enc, 0, El), ps=Rows(r.enc, g.X, El), pr=r.epr, xs=r.exs, xr=r.exr
    )

    def part_e(rows):
        return dot_nt(r.dckv[0, rows, :], r.wc[1]) + dot_nt(r.dckv[1, rows, :], r.wc[2])

    point()

    cm.ag_finish(2, v1)
    r.do[...] = dot_nt(r.dya[...], r.wo[...]).astype(BF)
    grad_out(r.sof, r.dya, r.ds.at[3])
    launch(t_s[3])
    point()
    state.drain_states()
    cm.rs_start_halves(3, ebuf, El, part_e)
    complete(t_1)
    gather(4, lambda s: r.g1.at[s], save_1)

    def between_self(a):
        if a == g.L // CH - 1:
            cm.ag_relay(*finals[0][:2])
            cm.rs_turn(3, ebuf)
        point()

    attend_backward(
        g,
        r.qkv.at[0],
        r.qkv.at[1],
        r.qkv.at[2],
        r.do,
        r.o_pbs,
        (r.pbuf, r.psem),
        (r.dqkv.at[0], r.dqkv.at[1], r.dqkv.at[2]),
        (r.dka, r.dva),
        g.L,
        True,
        between_self,
    )

    def part5(xx, dst):
        rows = at(xx * 2 * Tl, 2 * Tl)

        def body(n):
            cols = at(n * 256, 256)
            dst[:, cols] = (
                dot_nt(r.dqkv[0, rows, :], r.wq[0, cols, :])
                + dot_nt(r.dqkv[1, rows, :], r.wq[1, cols, :])
                + dot_nt(r.dqkv[2, rows, :], r.wq[2, cols, :])
            )

        loop(D // 256, body)

    l_x.wait()
    put_cols(0, colsum(r.dqkv[0]))
    put_cols(1, colsum(r.dqkv[2]))
    if g.wide:
        launch(t_g)
    for n in range(3):
        grad_rows(r.ds.at[n], r.x, r.dqkv.at[n])
        launch(t_s[n])
        point()
    cm.rs_start(2, buf, Tl, part5)
    cm.ag_relay(*finals[1][:2])
    complete([t_c[n] for n in (3, 1, 2, 0)])
    gather(5, lambda s: r.gc.at[s], save_n(r.gc, r.o_cq, r.o_co))
    r.ge[...] = cm.rs_finish(3, ebuf).astype(BF)
    save(r.ge, r.o_ge)
    r.gi[...] = (r.dh[...] + cm.rs_finish(2, buf)).astype(BF)
    save(r.gi, r.o_gi)
    order = [3, 0, 1, 2]
    for m, n in enumerate(order):
        complete([t_s[n]])
        gather(6 + n, lambda s, n=n: r.gs.at[s, n], save_n(r.gs, r.o_sq, r.o_so, [n]))
        cm.ag_relay(*finals[m + 2][:2])
        if n == 3 and g.wide:
            complete([t_g])
            cm.ag_start(10, lambda s: r.gg.at[s])
    cm.ag_relay(*finals[6][:2])
    v_gg = lambda s: r.gg.at[s]
    if g.wide:
        cm.ag_relay(10, v_gg)
        cm.ag_finish(10, v_gg)
    flush()
    if g.wide:
        total = r.gg[0]
        for s in range(1, g.S):
            total = total + r.gg[s]
        r.gsum[...] = total
        save(r.gsum, r.o_small)
    else:
        save(r.sg, r.o_small)
        save(r.fg, r.o_fg)

    cm.ag_drain(1, v2)
    cm.ag_drain(2, v1)
    for k, view, pairs in finals:
        cm.ag_drain(k, view)
    if g.wide:
        cm.ag_drain(10, v_gg)
    for t in tasks:
        cm.g_drain(t)
    state.drain()
    for d in outs + outs2:
        d.wait()


def whole_kernel(g, names, *refs):
    r = types.SimpleNamespace(**dict(zip(names, refs)))
    state = types.SimpleNamespace(outs=[])
    forward_body(g, r, Comm(g, r), state)
    backward_body(g, r, Comm(g, r, 6, 2 + g.D // 256), state)


def whole_call(g, ins):
    names, in_specs, args = [], [], []
    for n, a in ins.items():
        names.append(n)
        args.append(a)
        if n == LENS:
            in_specs.append(pl.BlockSpec(memory_space=pltpu.SMEM))
        elif a.size <= 8 * FJ_MAX:
            in_specs.append(pl.BlockSpec(memory_space=pltpu.VMEM))
        else:
            in_specs.append(ANY)
    D, L, E, Tl, El, S = g.D, g.L, g.E, g.Tl, g.El, g.S
    Dl, DH, FJ, FB = g.Dl, g.DH, g.FJ, g.FB
    V = pltpu.VMEM
    outs = dict(
        lo=((Tl, D), BF),
        x=((L, D), BF),
        pbs=((g.H, L, L), BF),
        pbc=((g.H, L, E), BF),
        gi=((Tl, D), BF),
        ge=((El, D), BF),
        f2=((g.FR, D), BF),
        f1=((Dl, g.FF) if g.wide else (S, Dl, FJ), BF),
        cq=((3, Dl, D), BF),
        co=((Dl, D), BF),
        sq=((3, Dl, D), BF),
        so=((Dl, D), BF),
        small=((NS, 128) if g.wide else (NS, D), F32),
    )
    if not g.wide:
        outs.update(fg=((8, FJ), F32))
    names += ["o_" + n for n in outs]
    scratch = dict(
        lo=V((Tl, D), BF),
        x=V((L, D), BF),
        enc=V((E, D), BF),
        wq=V((3, D, DH), BF),
        wo=V((DH, D), BF),
        wc=V((3, D, DH), BF),
        wd=V((DH, D), BF),
        w1=V((D, FJ), BF),
        w2=V((FJ, D), BF),
        sm=V((NS, D), F32),
        qkv=V((3, L, DH), BF),
        sof=V((S, L, DH), BF),
        fb=V((L, D), BF),
        cq=V((L, DH), BF),
        ckv=V((2, E, DH), BF),
        cof=V((S, L, DH), BF),
        hid=V((L, FJ), BF),
        dg=V((L, FJ), BF),
        h1=V((Tl, D), F32),
        h2=V((Tl, D), F32),
        h3=V((Tl, D), F32),
        rs1=V((Tl, 128), F32),
        rs2=V((Tl, 128), F32),
        rs3=V((Tl, 128), F32),
        bias=V((48, DH), F32),
        fbv=V((8, FJ), F32),
        gi=V((Tl, D), BF),
        ge=V((El, D), BF),
        g2=V((S, FB, D), BF),
        g1=V((S, Dl, FJ), BF),
        gc=V((S, 4, Dl, DH), BF),
        gs=V((S, 4, Dl, DH), BF),
        fsum=V((8, FJ), F32),
    )
    two = V((g.X, Tl, D), BF)
    one = V((g.X - 1, Tl, D), BF)
    scratch.update(
        og=V((Tl, D), BF),
        dh=V((Tl, D), F32),
        sg=V((NS, D), F32),
        part=V((2 * Tl, D), F32),
        acc=V((g.X, Tl, D), F32),
        ps=two,
        pr=two,
        xs=one,
        xr=one,
        epr=V((g.X, El, D), BF),
        exs=V((g.X - 1, El, D), BF),
        exr=V((g.X - 1, El, D), BF),
        dya=V((L, D), BF),
        dyb=V((L, D), BF),
        dpre=V((L, FJ), BF),
        do=V((L, DH), BF),
        dcq=V((L, DH), BF),
        dckv=V((2, E, DH), BF),
        dqkv=V((3, L, DH), BF),
        dka=V((g.NB, E, 128), F32),
        dva=V((g.NB, E, 128), F32),
        pbuf=V((2 * g.NB, CH, E), BF),
        d2=V((FJ, D), BF),
        d1=V((D, FJ), BF),
        dc=V((4, D, DH), BF),
        ds=V((4, D, DH), BF),
        yr2=V((D // 256, g.Y - 1, g.Z, FB, 256), BF),
        yr1=V((FJ // 256, g.Y - 1, g.Z, Dl, 256), BF),
        yrc=V((4, g.Y - 1, g.Z, Dl, DH), BF),
        yrs=V((4, g.Y - 1, g.Z, Dl, DH), BF),
        zr2=V((D // 256, g.Z - 1, FB, 256), BF),
        zr1=V((FJ // 256, g.Z - 1, Dl, 256), BF),
        zrc=V((4, g.Z - 1, Dl, DH), BF),
        zrs=V((4, g.Z - 1, Dl, DH), BF),
    )
    if not g.wide:
        scratch.update(fg=V((8, FJ), F32))
    if g.wide:
        scratch.update(
            smalls=V((g.R, NS, 128), BF),
            mine=V((NS, 128), F32),
            yrg=V((g.Y - 1, g.Z, NS, 128), F32),
            zrg=V((g.Z - 1, NS, 128), F32),
            gg=V((S, NS, 128), F32),
            gsum=V((NS, 128), F32),
        )
    sem = pltpu.SemaphoreType.DMA
    NP = 9 + FJ // 256 + D // 256
    scratch.update(
        ls=sem((10,)),
        lq=sem((g.NB,)),
        lc=sem((g.NB,)),
        l1=sem((g.R,)),
        wzs=sem((NP, g.Z - 1)),
        wzr=sem((NP, g.Z - 1)),
        wys=sem((NP, g.Y - 1, g.Z)),
        wyr=sem((NP, g.Y - 1, g.Z)),
        os=sem((8,)),
        psem=sem((2 * g.NB,)),
        fs=sem((7, max(S * (g.R if g.wide else 1), 4 * S * g.NB))),
        gys=sem((NP, g.Y - 1, g.Z)),
        gyr=sem((NP, g.Y - 1, g.Z)),
        gzs=sem((NP, g.Z - 1)),
        gzr=sem((NP, g.Z - 1)),
        axs=sem((17, g.X - 1)),
        axr=sem((17, g.X - 1)),
        acs=sem((17, g.X)),
        acr=sem((17, g.X)),
        rcs=sem((6 + D // 256, g.X)),
        rcr=sem((6 + D // 256, g.X)),
        rxs=sem((6 + D // 256, g.X - 1)),
        rxr=sem((6 + D // 256, g.X - 1)),
    )
    names += list(scratch)
    out = pl.pallas_call(
        functools.partial(whole_kernel, g, names),
        out_shape=[jax.ShapeDtypeStruct(*s) for s in outs.values()],
        in_specs=in_specs,
        out_specs=[ANY] * len(outs),
        scratch_shapes=list(scratch.values()),
        compiler_params=pltpu.CompilerParams(
            collective_id=0, has_side_effects=True, vmem_limit_bytes=67043328
        ),
    )(*args)
    return dict(zip(outs, out))


def finish_kernel(cuts, *refs):
    half = (len(refs) - len(cuts)) // 2
    ins, small = refs[:half], refs[half]
    outs, smalls = refs[half + 1 : 2 * half + 1], refs[2 * half + 1 :]
    for src, dst in zip(ins, outs):
        dst[...] = src[...].astype(dst.dtype)
    for (lo, hi), dst in zip(cuts, smalls):
        dst[...] = small[lo:hi, :]


def finish_call(g, parts, small):
    steps = 4 if g.Dl % 64 == 0 else 2
    nf = g.FF // g.D
    cuts = ((0, 6), (6, 6 + nf), (6 + nf, 7 + nf), (7 + nf, 10 + nf), (10 + nf, 13 + nf))
    specs, shapes = [], []
    for n, (a, dtype) in enumerate(parts):
        block = list(a.shape)
        block[-2] //= steps
        lead = a.ndim - 2
        specs.append(pl.BlockSpec(tuple(block), lambda k, lead=lead: (0,) * lead + (k, 0)))
        shapes.append(jax.ShapeDtypeStruct(a.shape, dtype))
    for lo, hi in cuts:
        shapes.append(jax.ShapeDtypeStruct((hi - lo, small.shape[1]), F32))

    def whole(shape):
        return pl.BlockSpec(shape, lambda k: (0, 0))

    return pl.pallas_call(
        functools.partial(finish_kernel, cuts),
        grid=(steps,),
        out_shape=shapes,
        in_specs=specs + [whole(small.shape)],
        out_specs=specs + [whole(s.shape) for s in shapes[len(specs) :]],
        compiler_params=pltpu.CompilerParams(vmem_limit_bytes=67043328),
    )(*[a for a, _ in parts], small)


def on_device(
    decoder_in,
    encoder_states,
    out_grad,
    seq_lengths,
    enc_lengths,
    self_qkv,
    self_out,
    cross_qkv,
    cross_out,
    attn_bias,
    ffn_in,
    ffn_in_bias,
    ffn_out,
    ffn_out_bias,
    norm_gain,
    norm_bias,
):
    R = lax.axis_size(DP)
    S = lax.axis_size(SEQ)
    j = lax.axis_index(SEQ)
    D = decoder_in.shape[2]
    FF = ffn_in.shape[1]
    g = configure(R, S, decoder_in.shape[1], encoder_states.shape[1], D, FF)
    Dl, FR, FB, FJ, NB = g.Dl, g.FR, g.FB, g.FJ, g.NB
    nf = FF // D
    nb = 6 + nf

    fi, fo = ffn_in_bias.reshape(nf, Dl), ffn_out_bias.reshape(1, Dl)
    lens = jnp.concatenate([seq_lengths, enc_lengths])
    ins = dict(
        lens=lens,
        tok=decoder_in[0],
        states=encoder_states[0],
        out_grad=out_grad[0],
        self_qkv=self_qkv,
        self_out=self_out,
        cross_qkv=cross_qkv,
        cross_out=cross_out,
        ffn_in=ffn_in,
        ffn_out=ffn_out,
    )
    if g.wide:
        ins.update(
            attn_bias=attn_bias,
            ffn_in_bias=fi,
            ffn_out_bias=fo,
            norm_gain=norm_gain,
            norm_bias=norm_bias,
        )
    else:
        pad = jnp.zeros((NS - nb - 7, Dl), BF)
        small = jnp.concatenate([attn_bias, fi, fo, norm_gain, norm_bias, pad])
        small = lax.all_gather(small, DP, axis=1, tiled=True)
        fb = small[6:nb].reshape(nf, R, Dl).transpose(1, 0, 2)
        fb = lax.dynamic_slice_in_dim(fb.reshape(R, FR), j * FB, FB, axis=1).reshape(1, -1)
        packed = lax.dynamic_slice_in_dim(ffn_in.reshape(Dl, R, FR), j * FB, FB, axis=2)
        ins.update(
            small=small,
            fbias=jnp.broadcast_to(fb.astype(F32), (8, FJ)),
            ffn_in=packed.reshape(Dl, FJ),
        )
    b = types.SimpleNamespace(**whole_call(g, ins))

    sm = b.small
    if not g.wide:
        fpl = lax.dynamic_update_slice(
            jnp.zeros((R, S, FB), F32), b.fg[0].reshape(R, 1, FB), (0, j, 0)
        )
        fpl = fpl.reshape(R, nf, Dl).transpose(1, 0, 2).reshape(nf, D)
        sm = lax.dynamic_update_slice(sm, fpl, (6, 0))
        sm = lax.psum(lax.psum_scatter(sm, DP, scatter_dimension=1, tiled=True), SEQ)

    gw1 = b.f1
    if not g.wide:
        gw1 = gw1.reshape(S, Dl, R, FB).transpose(1, 2, 0, 3).reshape(Dl, FF)
    parts = [(b.lo, BF), (b.gi, BF), (b.ge, BF)]
    parts += [(a, F32) for a in (b.sq, b.so, b.cq, b.co, gw1, b.f2)]
    lo, gi, ge, sq, so, cq, co, f1, f2, gab, gfi, gfo, ggain, gshift = finish_call(g, parts, sm)
    return (
        lo[None],
        gi[None],
        ge[None],
        sq,
        so,
        cq,
        co,
        gab,
        f1,
        gfi.reshape(-1),
        f2,
        gfo.reshape(-1),
        ggain,
        gshift,
    )


def solution(mesh):
    act = P(DP, SEQ, None)
    w3 = P(None, DP, None)
    w2 = P(DP, None)
    v2 = P(None, DP)
    v1 = P(DP)
    return jax.shard_map(
        on_device,
        mesh=mesh,
        in_specs=(act, act, act, v1, v1, w3, w2, w3, w2, v2, w2, v1, w2, v1, v2, v2),
        out_specs=(act, act, act, w3, w2, w3, w2, v2, w2, v1, w2, v1, v2, v2),
        check_vma=False,
    )
```
